32 devices in a mesh: dp: 8 (over z, x), tensor: 4 (over y, core).
Axes of the slice: x: 2, y: 2, z: 4, core: 2. Of those that a mesh axis runs over, the one named last changes fastest.
Arguments:
- tokens: float32 [160, 197, 768], P('dp'), may hold values from -6 to 6
- cotangent: float32 [160, 197, 768], P('dp'), may hold values from -6 to 6
- counts: int32 [8], P('dp'), may hold values from 1 to 20, 96 in all
- qkv_weight: float32 [768, 3, 768], P('dp', None, 'tensor'), may hold values from -1.6237976 to 1.6237976
- proj_weight: float32 [768, 768], P('tensor', 'dp'), may hold values from -0.75 to 0.75
- expand_weight: float32 [768, 3072], P('dp', 'tensor'), may hold values from -0.21875 to 0.21875
- reduce_weight: float32 [3072, 768], P('tensor', 'dp'), may hold values from -0.109375 to 0.109375
- qv_bias: float32 [2, 768], P(None, ('tensor', 'dp')), may hold values from -3 to 3
- expand_bias: float32 [3072], P(('tensor', 'dp')), may hold values from -3 to 3
- vectors: float32 [6, 768], P(None, 'dp'), may hold values from -1.25 to 2.5
- first_qkv_weight: float32 [768, 3, 768], P('dp', None, 'tensor'), may hold values from -24 to 24
- second_qkv_weight: float32 [768, 3, 768], P('dp', None, 'tensor'), may hold values from 3.7824 to 75.648
- first_proj_weight: float32 [768, 768], P('tensor', 'dp'), may hold values from -24 to 24
- second_proj_weight: float32 [768, 768], P('tensor', 'dp'), may hold values from 3.7824 to 75.648
- first_expand_weight: float32 [768, 3072], P('dp', 'tensor'), may hold values from -24 to 24
- second_expand_weight: float32 [768, 3072], P('dp', 'tensor'), may hold values from 3.7824 to 75.648
- first_reduce_weight: float32 [3072, 768], P('tensor', 'dp'), may hold values from -24 to 24
- second_reduce_weight: float32 [3072, 768], P('tensor', 'dp'), may hold values from 3.7824 to 75.648
- first_qv_bias: float32 [2, 768], P(None, ('tensor', 'dp')), may hold values from -24 to 24
- second_qv_bias: float32 [2, 768], P(None, ('tensor', 'dp')), may hold values from 3.7824 to 75.648
- first_expand_bias: float32 [3072], P(('tensor', 'dp')), may hold values from -24 to 24
- second_expand_bias: float32 [3072], P(('tensor', 'dp')), may hold values from 3.7824 to 75.648
- first_vectors: float32 [6, 768], P(None, 'dp'), may hold values from -24 to 24
- second_vectors: float32 [6, 768], P(None, 'dp'), may hold values from 3.7824 to 75.648
Outputs:
- output: float32 [160, 197, 768], P('dp', None, 'tensor')
- grad_tokens: float32 [160, 197, 768], P('dp', None, 'tensor')
- grad_qkv_weight: float32 [768, 3, 768], P('dp', None, 'tensor')
- new_qkv_weight: float32 [768, 3, 768], P('dp', None, 'tensor')
- new_first_qkv_weight: float32 [768, 3, 768], P('dp', None, 'tensor')
- new_second_qkv_weight: float32 [768, 3, 768], P('dp', None, 'tensor')
- grad_proj_weight: float32 [768, 768], P('tensor', 'dp')
- new_proj_weight: float32 [768, 768], P('tensor', 'dp')
- new_first_proj_weight: float32 [768, 768], P('tensor', 'dp')
- new_second_proj_weight: float32 [768, 768], P('tensor', 'dp')
- grad_expand_weight: float32 [768, 3072], P('dp', 'tensor')
- new_expand_weight: float32 [768, 3072], P('dp', 'tensor')
- new_first_expand_weight: float32 [768, 3072], P('dp', 'tensor')
- new_second_expand_weight: float32 [768, 3072], P('dp', 'tensor')
- grad_reduce_weight: float32 [3072, 768], P('tensor', 'dp')
- new_reduce_weight: float32 [3072, 768], P('tensor', 'dp')
- new_first_reduce_weight: float32 [3072, 768], P('tensor', 'dp')
- new_second_reduce_weight: float32 [3072, 768], P('tensor', 'dp')
- grad_qv_bias: float32 [2, 768], P(None, ('tensor', 'dp'))
- new_qv_bias: float32 [2, 768], P(None, ('tensor', 'dp'))
- new_first_qv_bias: float32 [2, 768], P(None, ('tensor', 'dp'))
- new_second_qv_bias: float32 [2, 768], P(None, ('tensor', 'dp'))
- grad_expand_bias: float32 [3072], P(('tensor', 'dp'))
- new_expand_bias: float32 [3072], P(('tensor', 'dp'))
- new_first_expand_bias: float32 [3072], P(('tensor', 'dp'))
- new_second_expand_bias: float32 [3072], P(('tensor', 'dp'))
- grad_vectors: float32 [6, 768], P(None, 'dp')
- new_vectors: float32 [6, 768], P(None, 'dp')
- new_first_vectors: float32 [6, 768], P(None, 'dp')
- new_second_vectors: float32 [6, 768], P(None, 'dp')
The draws below stay inside these ranges and needn't reach their ends.
Inputs may be any that keep to these rules, and one draw needn't show every extreme that they name: counts[i] of the 20 slots of data group i hold live images, the first ones; the counts sum to 96 and the largest is 20.
All inputs are finite; a program needn't handle non-finite values.
Results may differ from the reference program's by a relative error of at most 0.025.
The reference program's roundings to bfloat16 on the way count: a program that leaves them out, or rounds other values in their place, can miss the bound.
Values may be sent and summed in bfloat16 or wider, within the bound.
A program may use at most 320 MiB of HBM per device.

```python
import math
import jax
import jax.numpy as jnp
import numpy as np
from jax import lax

D = 768
HEADS = 12
FF = 3072
HEAD_DIM = 64
SEQ = 197
SLOTS = 20
IMAGES = 96
SLOTS_ALL = 160
N_DP = 8
N_TENSOR = 4


def draw_qkv_weight(key, part):
    keys = jax.random.split(key, 1)
    return jax.random.truncated_normal(keys[0], -3.0, 3.0, (D, 3, D), jnp.float32) * D ** (-0.5)


def draw_vectors(key, part):
    keys = jax.random.split(key, 2)
    gains = jnp.exp(0.3 * jax.random.truncated_normal(keys[0], -3.0, 3.0, (2, D), jnp.float32))
    shifts = 0.4 * jax.random.truncated_normal(keys[1], -3.0, 3.0, (4, D), jnp.float32)
    return jnp.stack([gains[0], shifts[0], shifts[1], gains[1], shifts[2], shifts[3]])


def levels(rng, extent, pieces, low, largest):
    factor_of, own = 1.0, jax.random.fold_in(rng, 6)
    for position, blocks in pieces:
        heights = jnp.exp(jax.random.uniform(jax.random.fold_in(own, position), (blocks,), jnp.float32, low / len(pieces), largest / len(pieces)))
        factor_of = factor_of * jnp.repeat(heights, extent[position] // blocks).reshape([-1 if axis == position else 1 for axis in range(len(extent))])
    return factor_of


def length_profile(count, total, most, slope):
    portions = [(1 << 20) // math.isqrt(rank ** slope) + 1 for rank in range(2, count + 1)]
    surplus, given = total - most - (count - 1), [1] * (count - 1)
    while surplus > 0:
        movable = [i for i in range(count - 1) if given[i] < most]
        pool, left = sum([portions[i] for i in movable]), surplus
        for i in movable:
            addition = min(most - given[i], max(1, left * portions[i] // pool), surplus)
            given[i] = given[i] + addition
            surplus = surplus - addition
    return np.array([most] + given)


def ragged(rng, number_of, total, limit, slope):
    if number_of == 2:
        one = jax.random.randint(rng, (), max(1, total - limit), min(limit, total - 1) + 1)
        return jnp.stack([one, total - one])
    sizes = jnp.asarray(length_profile(number_of, total, limit, slope), jnp.int32)
    twos = (number_of - 1) // 2
    source_of, sink = sizes[1:1 + 2 * twos:2], sizes[2:2 + 2 * twos:2]
    margin = jnp.minimum(source_of - 1, limit - sink)
    shifted = jax.random.randint(jax.random.fold_in(rng, 1), (twos,), 0, 1 << 20) % (margin + 1)
    sizes = sizes.at[1:1 + 2 * twos:2].set(source_of - shifted).at[2:2 + 2 * twos:2].set(sink + shifted)
    return sizes[jax.random.permutation(jax.random.fold_in(rng, 2), number_of)]


def gaussian(rng, dims, width, bound, cuts=(), held_as=jnp.bfloat16):
    drawn = jax.random.normal(rng, dims, jnp.float32) * width
    if len(cuts) > 0:
        drawn = levels(rng, dims, cuts, -0.22, 0.18) * drawn
    return jnp.clip(drawn, min=-bound, max=bound).astype(held_as)


def setup_inputs(seed: int = 0) -> dict:
    arg_keys = jax.random.split(jax.random.key(seed), 25)
    return {
        "tokens": gaussian(arg_keys[0], (SLOTS_ALL, SEQ, D), 1.0, 6.0, ((0, 8),), jnp.float32),
        "cotangent": gaussian(arg_keys[1], (SLOTS_ALL, SEQ, D), 1.0, 6.0, ((0, 8),), jnp.float32),
        "counts": ragged(arg_keys[2], N_DP, IMAGES, SLOTS, 1).astype(jnp.int32),
        "qkv_weight": draw_qkv_weight(jax.random.fold_in(arg_keys[24], 71), 0),
        "proj_weight": gaussian(arg_keys[4], (D, D), (D // 12) ** -0.5, 0.75, ((0, 4), (1, 8)), jnp.float32),
        "expand_weight": gaussian(arg_keys[5], (D, FF), D ** -0.5, 0.21875, ((0, 8), (1, 4)), jnp.float32),
        "reduce_weight": gaussian(arg_keys[6], (FF, D), FF ** -0.5, 0.109375, ((0, 4), (1, 8)), jnp.float32),
        "qv_bias": gaussian(arg_keys[7], (2, D), 0.5, 3.0, ((1, 32),), jnp.float32),
        "expand_bias": gaussian(arg_keys[8], (FF,), 0.5, 3.0, ((0, 32),), jnp.float32),
        "vectors": draw_vectors(jax.random.fold_in(arg_keys[24], 71), 0),
        "first_qkv_weight": gaussian(arg_keys[10], (D, 3, D), (0.03 * (IMAGES * SEQ) ** 0.5), 24.0, ((0, 8), (2, 4)), jnp.float32),
        "second_qkv_weight": jnp.clip(jnp.exp(math.log(75.648) - 2.9957323 * jax.random.uniform(arg_keys[11], (D, 3, D), jnp.float32) ** levels(arg_keys[11], (D, 3, D), ((0, 8), (2, 4)), -0.2, 0.2)), 3.7824, 75.648),
        "first_proj_weight": gaussian(arg_keys[12], (D, D), (0.03 * (IMAGES * SEQ) ** 0.5), 24.0, ((0, 4), (1, 8)), jnp.float32),
        "second_proj_weight": jnp.clip(jnp.exp(math.log(75.648) - 2.9957323 * jax.random.uniform(arg_keys[13], (D, D), jnp.float32) ** levels(arg_keys[13], (D, D), ((0, 4), (1, 8)), -0.2, 0.2)), 3.7824, 75.648),
        "first_expand_weight": gaussian(arg_keys[14], (D, FF), (0.03 * (IMAGES * SEQ) ** 0.5), 24.0, ((0, 8), (1, 4)), jnp.float32),
        "second_expand_weight": jnp.clip(jnp.exp(math.log(75.648) - 2.9957323 * jax.random.uniform(arg_keys[15], (D, FF), jnp.float32) ** levels(arg_keys[15], (D, FF), ((0, 8), (1, 4)), -0.2, 0.2)), 3.7824, 75.648),
        "first_reduce_weight": gaussian(arg_keys[16], (FF, D), (0.03 * (IMAGES * SEQ) ** 0.5), 24.0, ((0, 4), (1, 8)), jnp.float32),
        "second_reduce_weight": jnp.clip(jnp.exp(math.log(75.648) - 2.9957323 * jax.random.uniform(arg_keys[17], (FF, D), jnp.float32) ** levels(arg_keys[17], (FF, D), ((0, 4), (1, 8)), -0.2, 0.2)), 3.7824, 75.648),
        "first_qv_bias": gaussian(arg_keys[18], (2, D), (0.03 * (IMAGES * SEQ) ** 0.5), 24.0, ((1, 32),), jnp.float32),
        "second_qv_bias": jnp.clip(jnp.exp(math.log(75.648) - 2.9957323 * jax.random.uniform(arg_keys[19], (2, D), jnp.float32) ** levels(arg_keys[19], (2, D), ((1, 32),), -0.2, 0.2)), 3.7824, 75.648),
        "first_expand_bias": gaussian(arg_keys[20], (FF,), (0.03 * (IMAGES * SEQ) ** 0.5), 24.0, ((0, 32),), jnp.float32),
        "second_expand_bias": jnp.clip(jnp.exp(math.log(75.648) - 2.9957323 * jax.random.uniform(arg_keys[21], (FF,), jnp.float32) ** levels(arg_keys[21], (FF,), ((0, 32),), -0.2, 0.2)), 3.7824, 75.648),
        "first_vectors": gaussian(arg_keys[22], (6, D), (0.03 * (IMAGES * SEQ) ** 0.5), 24.0, ((1, 8),), jnp.float32),
        "second_vectors": jnp.clip(jnp.exp(math.log(75.648) - 2.9957323 * jax.random.uniform(arg_keys[23], (6, D), jnp.float32) ** levels(arg_keys[23], (6, D), ((1, 8),), -0.2, 0.2)), 3.7824, 75.648),
    }


lr_matrix = 0.006
lr_vector = 0.1
decay = 0.05
beta_one = 0.9
beta_two = 0.999
adam_eps = 1e-08
adam_step = 2.0
norm_eps = 1e-06

def rounded(value):
    return lax.optimization_barrier(value.astype(jnp.bfloat16)).astype(jnp.float32)

def layer_norm(rows, gain, shift):
    mean = lax.optimization_barrier(jnp.mean(rows, axis=-1, keepdims=True))
    centred = rows - mean
    variance = lax.optimization_barrier(jnp.mean(centred * centred, axis=-1, keepdims=True))
    scale = lax.rsqrt(variance + norm_eps)
    normed = centred * scale
    return (normed * gain + shift, normed, scale)

def norm_back(grad_in, normed, scale, gain):
    scaled = grad_in * gain
    return scale * (scaled - lax.optimization_barrier(jnp.mean(scaled, axis=-1, keepdims=True)) - normed * lax.optimization_barrier(jnp.mean(scaled * normed, axis=-1, keepdims=True)))

def gelu_exact(value):
    return jax.nn.gelu(value, approximate=False)

def grouped(spec, left, right):
    parts = jnp.einsum(spec, left.astype(jnp.float32), right.astype(jnp.float32))
    return lax.optimization_barrier(jnp.sum(rounded(parts), axis=0))

def adamw(master, grad, first, second, rate, decay_rate):
    first_new = beta_one * first + (1.0 - beta_one) * grad
    second_new = beta_two * second + (1.0 - beta_two) * grad * grad
    first_hat = first_new / (1.0 - beta_one ** adam_step)
    second_hat = second_new / (1.0 - beta_two ** adam_step)
    new = master - rate * (first_hat / (jnp.sqrt(second_hat) + adam_eps) + decay_rate * master)
    return (new, first_new, second_new)

def group_pass(params, tokens, cotangent, count):
    w_qkv, w_proj, w_expand, w_reduce, b_qv, b_expand, vec = params
    rows = SLOTS * SEQ
    local = D // N_TENSOR
    ff_local = FF // N_TENSOR
    scale_qk = HEAD_DIM ** (-0.5)
    f32 = jnp.float32
    bf16 = jnp.bfloat16
    live = (jnp.arange(SLOTS) < count).astype(f32)
    live_rows = jnp.broadcast_to(live[:, None], (SLOTS, SEQ)).reshape(rows, 1)
    flat = tokens.reshape(rows, D)
    a1, normed1, scale1 = layer_norm(flat, vec[0], vec[1])
    a1_half = a1.astype(bf16)
    qkv = jnp.dot(a1_half, w_qkv.reshape(D, 3 * D), preferred_element_type=f32).reshape(rows, 3, D)
    bias_f = b_qv.astype(f32)
    qkv = qkv + jnp.stack([bias_f[0], jnp.zeros((D,), f32), bias_f[1]])
    qkv_half = qkv.astype(bf16).reshape(SLOTS, SEQ, 3, HEADS, HEAD_DIM)
    query = qkv_half[:, :, 0].astype(f32)
    key = qkv_half[:, :, 1].astype(f32)
    value = qkv_half[:, :, 2].astype(f32)
    scores = jnp.einsum('sqhc,skhc->shqk', query, key) * scale_qk
    top = lax.optimization_barrier(jnp.max(scores, axis=-1, keepdims=True))
    lse = top + jnp.log(lax.optimization_barrier(jnp.sum(jnp.exp(scores - top), axis=-1, keepdims=True)))
    probs_f = jnp.exp(scores - lse)
    probs_half = probs_f.astype(bf16)
    mixed = jnp.einsum('shqk,skhc->sqhc', probs_half.astype(f32), value).astype(bf16).reshape(rows, D)
    attention = grouped('rtk,tkd->trd', mixed.reshape(rows, N_TENSOR, local), w_proj.reshape(N_TENSOR, local, D))
    resid = flat + attention + vec[2]
    a2, normed2, scale2 = layer_norm(resid, vec[3], vec[4])
    a2_half = a2.astype(bf16)
    pre = jnp.dot(a2_half, w_expand, preferred_element_type=f32) + b_expand.astype(f32)
    hidden = gelu_exact(pre).astype(bf16)
    feedforward = grouped('rtf,tfd->trd', hidden.reshape(rows, N_TENSOR, ff_local), w_reduce.reshape(N_TENSOR, ff_local, D))
    output = (resid + feedforward + vec[5]) * live_rows
    grad_out = cotangent.reshape(rows, D) * live_rows
    grad_half = grad_out.astype(bf16)
    d_reduce = jnp.dot(hidden.T, grad_half, preferred_element_type=f32)
    d_hidden = jnp.dot(grad_half, w_reduce.T, preferred_element_type=f32)
    unused, gelu_back = jax.vjp(gelu_exact, pre)
    d_pre = gelu_back(d_hidden)[0]
    d_expand_bias = lax.optimization_barrier(jnp.sum(d_pre, axis=0))
    d_pre_half = d_pre.astype(bf16)
    d_expand = jnp.dot(a2_half.T, d_pre_half, preferred_element_type=f32)
    d_a2 = grouped('rtf,dtf->trd', d_pre_half.reshape(rows, N_TENSOR, ff_local), w_expand.reshape(D, N_TENSOR, ff_local))
    d_resid = grad_out + norm_back(d_a2, normed2, scale2, vec[3])
    d_resid_half = d_resid.astype(bf16)
    d_proj = jnp.dot(mixed.T, d_resid_half, preferred_element_type=f32)
    d_mixed = jnp.dot(d_resid_half, w_proj.T, preferred_element_type=f32).astype(bf16)
    d_mixed = d_mixed.reshape(SLOTS, SEQ, HEADS, HEAD_DIM).astype(f32)
    d_value = jnp.einsum('shqk,sqhc->skhc', probs_half.astype(f32), d_mixed)
    d_probs = jnp.einsum('sqhc,skhc->shqk', d_mixed, value)
    delta = lax.optimization_barrier(jnp.sum(probs_f * d_probs, axis=-1, keepdims=True))
    d_scores = (probs_f * (d_probs - delta) * scale_qk).astype(bf16).astype(f32)
    d_query = jnp.einsum('shqk,skhc->sqhc', d_scores, key)
    d_key = jnp.einsum('shqk,sqhc->skhc', d_scores, query)
    d_qv_bias = jnp.stack([lax.optimization_barrier(jnp.sum(d_query.reshape(rows, D), axis=0)), lax.optimization_barrier(jnp.sum(d_value.reshape(rows, D), axis=0))])
    d_qkv_half = jnp.stack([d_query, d_key, d_value], axis=2).astype(bf16).reshape(rows, 3, D)
    d_qkv = jnp.dot(a1_half.T, d_qkv_half.reshape(rows, 3 * D), preferred_element_type=f32).reshape(D, 3, D)
    d_a1 = grouped('rjtc,djtc->trd', d_qkv_half.reshape(rows, 3, N_TENSOR, local), w_qkv.reshape(D, 3, N_TENSOR, local))
    d_flat = d_resid + norm_back(d_a1, normed1, scale1, vec[0])
    d_vectors = jnp.stack([lax.optimization_barrier(jnp.sum(d_a1 * normed1, axis=0)), lax.optimization_barrier(jnp.sum(d_a1, axis=0)), lax.optimization_barrier(jnp.sum(d_resid, axis=0)), lax.optimization_barrier(jnp.sum(d_a2 * normed2, axis=0)), lax.optimization_barrier(jnp.sum(d_a2, axis=0)), lax.optimization_barrier(jnp.sum(grad_out, axis=0))])
    grads = (d_qkv, d_proj, d_expand, d_reduce, d_qv_bias, d_expand_bias, d_vectors)
    return (output.reshape(SLOTS, SEQ, D), d_flat.reshape(SLOTS, SEQ, D), grads)

def reference(tokens, cotangent, counts, qkv_weight, proj_weight, expand_weight, reduce_weight, qv_bias, expand_bias, vectors, first_qkv_weight, second_qkv_weight, first_proj_weight, second_proj_weight, first_expand_weight, second_expand_weight, first_reduce_weight, second_reduce_weight, first_qv_bias, second_qv_bias, first_expand_bias, second_expand_bias, first_vectors, second_vectors):
    masters = (qkv_weight, proj_weight, expand_weight, reduce_weight, qv_bias, expand_bias, vectors)
    halves = lax.optimization_barrier(tuple((w.astype(jnp.bfloat16) for w in masters)))
    params = halves[:6] + (halves[6].astype(jnp.float32),)
    zeros = tuple((jnp.zeros(w.shape, jnp.float32) for w in masters))

    def one_group(carry, block):
        tok, cot, count = block
        out, d_flat, grads = group_pass(params, tok, cot, count)
        return (tuple((a + b for a, b in zip(carry, grads))), (out, d_flat))
    grads, stacked = lax.scan(one_group, zeros, (tokens.reshape(N_DP, SLOTS, SEQ, D), cotangent.reshape(N_DP, SLOTS, SEQ, D), counts))
    output = stacked[0].reshape(SLOTS_ALL, SEQ, D)
    grad_tokens = stacked[1].reshape(SLOTS_ALL, SEQ, D)
    g_qkv, g_proj, g_expand, g_reduce, g_qvb, g_expb, g_vec = grads
    n_qkv, f_qkv, s_qkv = adamw(qkv_weight, g_qkv, first_qkv_weight, second_qkv_weight, lr_matrix, decay)
    n_proj, f_proj, s_proj = adamw(proj_weight, g_proj, first_proj_weight, second_proj_weight, lr_matrix, decay)
    n_expand, f_expand, s_expand = adamw(expand_weight, g_expand, first_expand_weight, second_expand_weight, lr_matrix, decay)
    n_reduce, f_reduce, s_reduce = adamw(reduce_weight, g_reduce, first_reduce_weight, second_reduce_weight, lr_matrix, decay)
    n_qvb, f_qvb, s_qvb = adamw(qv_bias, g_qvb, first_qv_bias, second_qv_bias, lr_vector, 0.0)
    n_expb, f_expb, s_expb = adamw(expand_bias, g_expb, first_expand_bias, second_expand_bias, lr_vector, 0.0)
    n_vec, f_vec, s_vec = adamw(vectors, g_vec, first_vectors, second_vectors, lr_vector, 0.0)
    return (output, grad_tokens, g_qkv, n_qkv, f_qkv, s_qkv, g_proj, n_proj, f_proj, s_proj, g_expand, n_expand, f_expand, s_expand, g_reduce, n_reduce, f_reduce, s_reduce, g_qvb, n_qvb, f_qvb, s_qvb, g_expb, n_expb, f_expb, s_expb, g_vec, n_vec, f_vec, s_vec)
```

```python
import functools

import jax
import jax.numpy as jnp
from jax import lax
from jax.experimental import pallas as pl
from jax.experimental.pallas import tpu as pltpu
from jax.sharding import PartitionSpec as P

HEAD_DIM = 64
f32 = jnp.float32
bf16 = jnp.bfloat16

lr_matrix = 0.006
lr_vector = 0.1
decay = 0.05
beta_one = 0.9
beta_two = 0.999
adam_eps = 1e-08
adam_step = 2.0
norm_eps = 1e-06
SMALL_ROWS = 16
VMEM_MAX = 63 * 1024 * 1024


def dot_nn(a, b):
    return lax.dot_general(a, b, (((1,), (0,)), ((), ())), preferred_element_type=f32)


def dot_nt(a, b):
    return lax.dot_general(a, b, (((1,), (1,)), ((), ())), preferred_element_type=f32)


def dot_tn(a, b):
    return lax.dot_general(a, b, (((0,), (0,)), ((), ())), preferred_element_type=f32)


def half_round(v):
    return v.astype(bf16).astype(f32)


def norm_stats(rows):
    mean = jnp.mean(rows, axis=-1, keepdims=True)
    centred = rows - mean
    variance = jnp.mean(centred * centred, axis=-1, keepdims=True)
    scale = lax.rsqrt(variance + norm_eps)
    return centred * scale, scale


def norm_back(grad_in, normed, scale, gain):
    scaled = grad_in * gain
    return scale * (
        scaled
        - jnp.mean(scaled, axis=-1, keepdims=True)
        - normed * jnp.mean(scaled * normed, axis=-1, keepdims=True)
    )


def places(n_z):
    dp = lax.axis_index("dp")
    t = lax.axis_index("tensor")
    z, x = dp // 2, dp % 2
    y, c = t // 2, t % 2
    fy, fx = 1 - 2 * y, 1 - 2 * x
    first = (dp + c * fx, t + (1 - c) * 2 * fy)
    second = (dp + (1 - c) * fx, t + c * 2 * fy)
    sibling = (dp, t + 1 - 2 * c)
    sets = (
        (y, x),
        (y + (1 - c) * fy, x + c * fx),
        (y + c * fy, x + (1 - c) * fx),
        (1 - y, 1 - x),
    )
    along_z = [(lax.rem(z + k, n_z) * 2 + x, t) for k in range(1, n_z)]
    return z, x, y, c, first, second, sibling, sets, along_z


def greet(peers):
    barrier = pltpu.get_barrier_semaphore()
    for peer in peers:
        pl.semaphore_signal(barrier, inc=1, device_id=peer, device_id_type=pl.DeviceIdType.MESH)
    pl.semaphore_wait(barrier, len(peers))


def push(src, dst, send, recv, peer):
    return pltpu.make_async_remote_copy(
        src_ref=src,
        dst_ref=dst,
        send_sem=send,
        recv_sem=recv,
        device_id=peer,
        device_id_type=pl.DeviceIdType.MESH,
    )


def gather_body(n_w, n_z, *refs):
    shards, outs = refs[:n_w], refs[n_w : 2 * n_w]
    local_sem, z_send, z_recv, s_send, s_recv = refs[2 * n_w :]
    z, x, y, c, first, second, sibling, sets, along_z = places(n_z)
    greet([first, second, sibling] + along_z)

    def own(w):
        return pltpu.make_async_copy(shards[w], outs[w].at[y, c, z, x], local_sem.at[w])

    def to_z(w, k):
        return push(shards[w], outs[w].at[y, c, z, x], z_send.at[w, k], z_recv.at[w, k], along_z[k])

    def move(w, which, peer, slot):
        sy, sx = sets[which]
        part = outs[w].at[sy, c, :, sx]
        return push(part, part, s_send.at[w, slot], s_recv.at[w, slot], peer)

    plan = {
        0: (0, first),
        1: (0, second),
        2: (1, second),
        3: (0, sibling),
        4: (1, sibling),
        5: (2, sibling),
        6: (3, sibling),
    }

    def go(w, slot):
        which, peer = plan[slot]
        move(w, which, peer, slot).start()

    def arrived(w, slot):
        which, peer = plan[slot]
        move(w, which, peer, slot).wait_recv()

    for w in range(n_w):
        own(w).start()
        for k in range(n_z - 1):
            to_z(w, k).start()
    for step in range(n_w + 3):
        w = step
        if 0 <= w < n_w:
            own(w).wait()
            for k in range(n_z - 1):
                to_z(w, k).wait_recv()
            for slot in (0, 1, 3):
                go(w, slot)
        w = step - 1
        if 0 <= w < n_w:
            arrived(w, 0)
            go(w, 2)
            go(w, 4)
        w = step - 2
        if 0 <= w < n_w:
            arrived(w, 1)
            go(w, 5)
            arrived(w, 2)
            go(w, 6)
        w = step - 3
        if 0 <= w < n_w:
            for slot in (3, 4, 5, 6):
                arrived(w, slot)
    for w in range(n_w):
        for k in range(n_z - 1):
            to_z(w, k).wait_send()
        for slot, (which, peer) in plan.items():
            move(w, which, peer, slot).wait_send()


def gather_all(shards, n_dp):
    n_w, n_z = len(shards), n_dp // 2
    shapes = [(2, 2, n_z, 2) + s.shape for s in shards]
    return pl.pallas_call(
        functools.partial(gather_body, n_w, n_z),
        out_shape=[jax.ShapeDtypeStruct(s, bf16) for s in shapes],
        in_specs=[pl.BlockSpec(memory_space=pltpu.VMEM)] * n_w,
        out_specs=[pl.BlockSpec(memory_space=pl.ANY)] * n_w,
        scratch_shapes=[
            pltpu.SemaphoreType.DMA((n_w,)),
            pltpu.SemaphoreType.DMA((n_w, n_z - 1)),
            pltpu.SemaphoreType.DMA((n_w, n_z - 1)),
            pltpu.SemaphoreType.DMA((n_w, 7)),
            pltpu.SemaphoreType.DMA((n_w, 7)),
        ],
        compiler_params=pltpu.CompilerParams(collective_id=0, has_side_effects=True),
        name="gather_weights",
    )(*shards)


def reduce_body(n_w, n_z, widths, *refs):
    grads, outs = refs[:n_w], refs[n_w : 2 * n_w]
    acc, got = refs[2 * n_w : 3 * n_w], refs[3 * n_w : 4 * n_w]
    got2, got1, gotz = refs[4 * n_w : 5 * n_w], refs[5 * n_w : 6 * n_w], refs[6 * n_w : 7 * n_w]
    local_sem, c_send, c_recv, s_send, s_recv, z_send, z_recv = refs[7 * n_w :]
    z, x, y, c, first, second, sibling, sets, along_z = places(n_z)
    greet([first, second, sibling] + along_z)
    swap = (0, 2, 1, 3)

    def part(w, which, core):
        sy, sx = sets[which]
        lanes = pl.ds(pl.multiple_of((sy * 2 + core) * widths[w], 128), widths[w])
        return grads[w].at[:, sx, :, lanes]

    def mine(w, k):
        return pltpu.make_async_copy(part(w, k, c), acc[w].at[k], local_sem.at[w, k])

    def to_sibling(w, k):
        s = swap[k]
        return push(part(w, k, 1 - c), got[w].at[s], c_send.at[w, s], c_recv.at[w, s], sibling)

    def to_second(w, k):
        return push(acc[w].at[k], got2[w].at[k - 2], s_send.at[w, k - 2], s_recv.at[w, k - 2], second)

    def to_first(w):
        return push(acc[w].at[1], got1[w], s_send.at[w, 2], s_recv.at[w, 2], first)

    def to_z(w, k):
        return push(
            acc[w].at[0, along_z[k][0] // 2], gotz[w].at[k], z_send.at[w, k], z_recv.at[w, k], along_z[k]
        )

    def add(w, k, other):
        def one(i, carry):
            acc[w][k, i] = (acc[w][k, i].astype(f32) + other(i).astype(f32)).astype(bf16)
            return carry

        lax.fori_loop(0, n_z, one, 0)

    for w in range(n_w):
        for k in (3, 1, 2, 0):
            to_sibling(w, k).start()
        for k in (3, 2, 1, 0):
            mine(w, k).start()
    for step in range(n_w + 3):
        w = step
        if 0 <= w < n_w:
            for k in (3, 2, 1, 0):
                mine(w, k).wait()
                to_sibling(w, swap[k]).wait_recv()
                add(w, k, lambda i, k=k: got[w][k, i])
                if k >= 2:
                    to_second(w, k).start()
        w = step - 1
        if 0 <= w < n_w:
            to_second(w, 3).wait_recv()
            add(w, 1, lambda i: got2[w][1, i])
            to_first(w).start()
            to_second(w, 2).wait_recv()
            add(w, 0, lambda i: got2[w][0, i])
        w = step - 2
        if 0 <= w < n_w:
            to_first(w).wait_recv()
            add(w, 0, lambda i: got1[w][i])
            for k in range(n_z - 1):
                to_z(w, k).start()
        w = step - 3
        if 0 <= w < n_w:
            total = acc[w][0, z].astype(f32)
            for k in range(n_z - 1):
                to_z(w, k).wait_recv()
                total = total + gotz[w][k].astype(f32)
            outs[w][...] = total
    for w in range(n_w):
        for k in range(4):
            to_sibling(w, k).wait_send()
        to_second(w, 2).wait_send()
        to_second(w, 3).wait_send()
        to_first(w).wait_send()
        for k in range(n_z - 1):
            to_z(w, k).wait_send()


def reduce_all(grads, widths, n_dp):
    n_w, n_z = len(grads), n_dp // 2
    rows = [g.shape[0] // n_dp for g in grads]
    shaped = [g.reshape(n_z, 2, r, g.shape[1]) for g, r in zip(grads, rows)]
    blocks = list(zip(rows, widths))
    scratch = [pltpu.VMEM((4, n_z) + b, bf16) for b in blocks]
    scratch += [pltpu.VMEM((4, n_z) + b, bf16) for b in blocks]
    scratch += [pltpu.VMEM((2, n_z) + b, bf16) for b in blocks]
    scratch += [pltpu.VMEM((n_z,) + b, bf16) for b in blocks]
    scratch += [pltpu.VMEM((n_z - 1,) + b, bf16) for b in blocks]
    scratch += [pltpu.SemaphoreType.DMA((n_w, 4))] * 3
    scratch += [pltpu.SemaphoreType.DMA((n_w, 3))] * 2
    scratch += [pltpu.SemaphoreType.DMA((n_w, n_z - 1))] * 2
    return pl.pallas_call(
        functools.partial(reduce_body, n_w, n_z, tuple(widths)),
        out_shape=[jax.ShapeDtypeStruct(b, f32) for b in blocks],
        in_specs=[pl.BlockSpec(memory_space=pl.ANY)] * n_w,
        out_specs=[pl.BlockSpec(memory_space=pltpu.VMEM)] * n_w,
        scratch_shapes=scratch,
        compiler_params=pltpu.CompilerParams(
            collective_id=1, has_side_effects=True, vmem_limit_bytes=VMEM_MAX
        ),
        name="reduce_grads",
    )(*shaped)


def key_mask(rows, seq):
    return lax.broadcasted_iota(jnp.int32, (rows, rows), 1) < seq


def load_rows(src, dst, seq):
    dst[pl.ds(0, seq), :] = src[0]


def front_body(seq, n_heads, where, x_ref, vec_ref, bias_ref, wq_ref, a1_ref, qkv_ref, mix_ref, lse_ref, xs):
    rows = xs.shape[0]

    @pl.when(pl.program_id(0) == 0)
    def _():
        xs[...] = jnp.zeros_like(xs)

    load_rows(x_ref, xs, seq)
    normed, unused = norm_stats(xs[...])
    a1 = (normed * vec_ref[0:1, :] + vec_ref[1:2, :]).astype(bf16)
    a1_ref[...] = a1
    mask = key_mask(rows, seq)
    lane = lax.broadcasted_iota(jnp.int32, (rows, 128), 1)
    lse_ref[...] = jnp.zeros_like(lse_ref)
    q_width = n_heads * HEAD_DIM
    wide = bias_ref.shape[2]
    pad = mix_ref.shape[1] // 4 - q_width
    for t in range(4):
        qkv = (dot_nn(a1_ref[...], wq_ref[t, :, :wide]) + bias_ref[t, 0:1, :]).astype(bf16)
        qkv_ref[:, t * wide : (t + 1) * wide] = qkv
        outs = [jnp.zeros((rows, pad), bf16)]
        for h in range(n_heads):
            q = qkv[:, h * HEAD_DIM : (h + 1) * HEAD_DIM]
            k = qkv[:, q_width + h * HEAD_DIM : q_width + (h + 1) * HEAD_DIM]
            v = qkv[:, 2 * q_width + h * HEAD_DIM : 2 * q_width + (h + 1) * HEAD_DIM]
            s = jnp.where(mask, dot_nt(q, k) * (HEAD_DIM**-0.5), -1e30)
            top = jnp.max(s, axis=-1, keepdims=True)
            e = jnp.exp(s - top)
            total = jnp.sum(e, axis=-1, keepdims=True)
            p = (e * (1.0 / total)).astype(bf16)
            outs.append(dot_nn(p, v).astype(bf16))
            lse = top + jnp.log(total)
            lse_ref[...] = jnp.where(lane == t * n_heads + h, lse, lse_ref[...])
        mix_ref[:, t * (pad + q_width) : (t + 1) * (pad + q_width)] = jnp.concatenate(outs, axis=1)


def front(where, tokens, vec, bias, wq, n_img, rows, n_heads):
    slots, seq, width = tokens.shape
    wide = bias.shape[2]
    mix = width - (3 * n_heads * HEAD_DIM // 128) * 128
    total = n_img * rows
    return pl.pallas_call(
        functools.partial(front_body, seq, n_heads),
        out_shape=[
            jax.ShapeDtypeStruct((total, width), bf16),
            jax.ShapeDtypeStruct((total, 4 * wide), bf16),
            jax.ShapeDtypeStruct((total, 4 * mix), bf16),
            jax.ShapeDtypeStruct((total, 128), f32),
        ],
        grid_spec=pltpu.PrefetchScalarGridSpec(
            num_scalar_prefetch=1,
            grid=(n_img,),
            in_specs=[
                pl.BlockSpec((1, seq, width), lambda i, s: (s[0] + i, 0, 0)),
                pl.BlockSpec(vec.shape, lambda i, s: (0, 0)),
                pl.BlockSpec(bias.shape, lambda i, s: (0, 0, 0)),
                pl.BlockSpec(wq.shape, lambda i, s: (0, 0, 0), pipeline_mode=pl.Buffered(1)),
            ],
            out_specs=[
                pl.BlockSpec((rows, width), lambda i, s: (i, 0)),
                pl.BlockSpec((rows, 4 * wide), lambda i, s: (i, 0)),
                pl.BlockSpec((rows, 4 * mix), lambda i, s: (i, 0)),
                pl.BlockSpec((rows, 128), lambda i, s: (i, 0)),
            ],
            scratch_shapes=[pltpu.VMEM((rows, width), f32)],
        ),
        compiler_params=pltpu.CompilerParams(vmem_limit_bytes=VMEM_MAX),
        name="front",
    )(where, tokens, vec, bias, wq)


def middle_body(
    seq,
    where,
    x_ref,
    cot_ref,
    mix_ref,
    vec_ref,
    bexp_ref,
    wq_ref,
    we_ref,
    wr_ref,
    a2_ref,
    hid_ref,
    dpre_ref,
    gh_ref,
    dres_ref,
    drh_ref,
    dmix_ref,
    out_ref,
    dvec_ref,
    dbexp_ref,
    xs,
    gs,
):
    i = pl.program_id(0)

    @pl.when(i == 0)
    def _():
        xs[...] = jnp.zeros_like(xs)
        gs[...] = jnp.zeros_like(gs)
        dvec_ref[...] = jnp.zeros_like(dvec_ref)
        dbexp_ref[...] = jnp.zeros_like(dbexp_ref)

    live = jnp.where(where[0] + i < where[1], 1.0, 0.0).astype(f32)
    load_rows(x_ref, xs, seq)
    gs[pl.ds(0, seq), :] = cot_ref[0] * live
    rows, width = xs.shape
    mix = mix_ref.shape[1] // 4
    ff = we_ref.shape[2]
    att = jnp.zeros((rows, width), f32)
    for t in range(4):
        att += half_round(dot_nt(mix_ref[:, t * mix : (t + 1) * mix], wq_ref[t, :, width - mix :]))
    resid = xs[...] + att + vec_ref[2:3, :]
    normed2, scale2 = norm_stats(resid)
    a2_ref[...] = (normed2 * vec_ref[3:4, :] + vec_ref[4:5, :]).astype(bf16)
    gh_ref[...] = gs[...].astype(bf16)
    feed = jnp.zeros((rows, width), f32)
    d_a2 = jnp.zeros((rows, width), f32)
    for t in range(4):
        pre = dot_nn(a2_ref[...], we_ref[t]) + bexp_ref[t, 0:1, :]
        cdf = 0.5 + 0.5 * lax.erf(pre * (0.5**0.5))
        hid = (pre * cdf).astype(bf16)
        slope = cdf + pre * jnp.exp(-0.5 * pre * pre) * ((2.0 * jnp.pi) ** -0.5)
        hid_ref[:, t * ff : (t + 1) * ff] = hid
        d_pre = dot_nn(gh_ref[...], wr_ref[t]) * slope
        dbexp_ref[t, 0:1, :] += jnp.sum(d_pre, axis=0, keepdims=True)
        dph = d_pre.astype(bf16)
        dpre_ref[:, t * ff : (t + 1) * ff] = dph
        feed += half_round(dot_nt(hid, wr_ref[t]))
        d_a2 += half_round(dot_nt(dph, we_ref[t]))
    out = (resid + feed + vec_ref[5:6, :]) * live
    col = width // 4
    for t in range(4):
        out_ref[t, 0] = out[:seq, t * col : (t + 1) * col].astype(bf16)
    d_resid = gs[...] + norm_back(d_a2, normed2, scale2, vec_ref[3:4, :])
    dres_ref[...] = d_resid
    drh = d_resid.astype(bf16)
    drh_ref[...] = drh
    for t in range(4):
        dmix_ref[:, t * mix : (t + 1) * mix] = dot_nn(drh, wq_ref[t, :, width - mix :]).astype(bf16)
    dvec_ref[2:3, :] += jnp.sum(d_resid, axis=0, keepdims=True)
    dvec_ref[3:4, :] += jnp.sum(d_a2 * normed2, axis=0, keepdims=True)
    dvec_ref[4:5, :] += jnp.sum(d_a2, axis=0, keepdims=True)
    dvec_ref[5:6, :] += jnp.sum(gs[...], axis=0, keepdims=True)


def middle(where, tokens, cotangent, mixp, vec, bexp, wq, we, wr, n_img, rows):
    slots, seq, width = tokens.shape
    ff = we.shape[2]
    mix = mixp.shape[1]
    total = n_img * rows
    col = width // 4
    row_block = lambda n: pl.BlockSpec((rows, n), lambda i, s: (i, 0))
    whole = lambda a: pl.BlockSpec(
        a.shape, lambda i, s, nd=len(a.shape): (0,) * nd, pipeline_mode=pl.Buffered(1)
    )
    image = pl.BlockSpec((1, seq, width), lambda i, s: (s[0] + i, 0, 0))
    return pl.pallas_call(
        functools.partial(middle_body, seq),
        out_shape=[
            jax.ShapeDtypeStruct((total, width), bf16),
            jax.ShapeDtypeStruct((total, 4 * ff), bf16),
            jax.ShapeDtypeStruct((total, 4 * ff), bf16),
            jax.ShapeDtypeStruct((total, width), bf16),
            jax.ShapeDtypeStruct((total, width), f32),
            jax.ShapeDtypeStruct((total, width), bf16),
            jax.ShapeDtypeStruct((total, mix), bf16),
            jax.ShapeDtypeStruct((4, n_img, seq, col), bf16),
            jax.ShapeDtypeStruct((8, width), f32),
            jax.ShapeDtypeStruct((4, 8, ff), f32),
        ],
        grid_spec=pltpu.PrefetchScalarGridSpec(
            num_scalar_prefetch=1,
            grid=(n_img,),
            in_specs=[image, image, row_block(mix)] + [whole(a) for a in (vec, bexp, wq, we, wr)],
            out_specs=[
                row_block(width),
                row_block(4 * ff),
                row_block(4 * ff),
                row_block(width),
                row_block(width),
                row_block(width),
                row_block(mix),
                pl.BlockSpec((4, 1, seq, col), lambda i, s: (0, i, 0, 0)),
                pl.BlockSpec((8, width), lambda i, s: (0, 0)),
                pl.BlockSpec((4, 8, ff), lambda i, s: (0, 0, 0)),
            ],
            scratch_shapes=[pltpu.VMEM((rows, width), f32), pltpu.VMEM((rows, width), f32)],
        ),
        compiler_params=pltpu.CompilerParams(vmem_limit_bytes=VMEM_MAX),
        name="middle",
    )(where, tokens, cotangent, mixp, vec, bexp, wq, we, wr)


def back_body(
    seq,
    n_heads,
    where,
    x_ref,
    qkv_ref,
    lse_ref,
    dmix_ref,
    dres_ref,
    vec_ref,
    wq_ref,
    dqkv_ref,
    gt_ref,
    dvec_ref,
    dbias_ref,
    xs,
):
    i = pl.program_id(0)

    @pl.when(i == 0)
    def _():
        xs[...] = jnp.zeros_like(xs)
        dvec_ref[...] = jnp.zeros_like(dvec_ref)
        dbias_ref[...] = jnp.zeros_like(dbias_ref)

    load_rows(x_ref, xs, seq)
    rows, width = xs.shape
    mask = key_mask(rows, seq)
    q_width = n_heads * HEAD_DIM
    wide = qkv_ref.shape[1] // 4
    mix = dmix_ref.shape[1] // 4
    scale_qk = HEAD_DIM**-0.5
    d_a1 = jnp.zeros((rows, width), f32)
    for t in range(4):
        dq, dk, dv = [], [], []
        for h in range(n_heads):
            at = t * wide + h * HEAD_DIM
            q = qkv_ref[:, at : at + HEAD_DIM]
            k = qkv_ref[:, at + q_width : at + q_width + HEAD_DIM]
            v = qkv_ref[:, at + 2 * q_width : at + 2 * q_width + HEAD_DIM]
            m_at = (t + 1) * mix - q_width + h * HEAD_DIM
            dm = dmix_ref[:, m_at : m_at + HEAD_DIM]
            lse = lse_ref[:, t * n_heads + h : t * n_heads + h + 1]
            p = jnp.where(mask, jnp.exp(dot_nt(q, k) * scale_qk - lse), 0.0)
            dv.append(dot_tn(p.astype(bf16), dm))
            d_p = dot_nt(dm, v)
            delta = jnp.sum(p * d_p, axis=-1, keepdims=True)
            ds = (p * (d_p - delta) * scale_qk).astype(bf16)
            dq.append(dot_nn(ds, k))
            dk.append(dot_tn(ds, q))
        d_all = jnp.concatenate(dq + dk + dv + [jnp.zeros((rows, wide - 3 * q_width), f32)], axis=1)
        dbias_ref[t, 0:1, :] += jnp.sum(d_all, axis=0, keepdims=True)
        d_half = d_all.astype(bf16)
        dqkv_ref[:, t * wide : (t + 1) * wide] = d_half
        d_a1 += half_round(dot_nt(d_half, wq_ref[t, :, :wide]))
    normed, scale = norm_stats(xs[...])
    grad = dres_ref[...] + norm_back(d_a1, normed, scale, vec_ref[0:1, :])
    col = width // 4
    for t in range(4):
        gt_ref[t, 0] = grad[:seq, t * col : (t + 1) * col].astype(bf16)
    dvec_ref[0:1, :] += jnp.sum(d_a1 * normed, axis=0, keepdims=True)
    dvec_ref[1:2, :] += jnp.sum(d_a1, axis=0, keepdims=True)


def back(where, tokens, qkv, lse, dmix, dres, vec, wq, n_img, rows, n_heads):
    slots, seq, width = tokens.shape
    total = n_img * rows
    wide = qkv.shape[1] // 4
    col = width // 4
    row_block = lambda n: pl.BlockSpec((rows, n), lambda i, s: (i, 0))
    whole = lambda a: pl.BlockSpec(
        a.shape, lambda i, s, nd=len(a.shape): (0,) * nd, pipeline_mode=pl.Buffered(1)
    )
    return pl.pallas_call(
        functools.partial(back_body, seq, n_heads),
        out_shape=[
            jax.ShapeDtypeStruct((total, 4 * wide), bf16),
            jax.ShapeDtypeStruct((4, n_img, seq, col), bf16),
            jax.ShapeDtypeStruct((8, width), f32),
            jax.ShapeDtypeStruct((4, 8, wide), f32),
        ],
        grid_spec=pltpu.PrefetchScalarGridSpec(
            num_scalar_prefetch=1,
            grid=(n_img,),
            in_specs=[
                pl.BlockSpec((1, seq, width), lambda i, s: (s[0] + i, 0, 0)),
                row_block(4 * wide),
                row_block(128),
                row_block(dmix.shape[1]),
                row_block(width),
                whole(vec),
                whole(wq),
            ],
            out_specs=[
                row_block(4 * wide),
                pl.BlockSpec((4, 1, seq, col), lambda i, s: (0, i, 0, 0)),
                pl.BlockSpec((8, width), lambda i, s: (0, 0)),
                pl.BlockSpec((4, 8, wide), lambda i, s: (0, 0, 0)),
            ],
            scratch_shapes=[pltpu.VMEM((rows, width), f32)],
        ),
        compiler_params=pltpu.CompilerParams(vmem_limit_bytes=VMEM_MAX),
        name="back",
    )(where, tokens, qkv, lse, dmix, dres, vec, wq)


def adamw(master, grad, first, second, rate, decay_rate):
    first_new = beta_one * first + (1.0 - beta_one) * grad
    second_new = beta_two * second + (1.0 - beta_two) * grad * grad
    first_hat = first_new / (1.0 - beta_one**adam_step)
    second_hat = second_new / (1.0 - beta_two**adam_step)
    new = master - rate * (first_hat / (jnp.sqrt(second_hat) + adam_eps) + decay_rate * master)
    return (new, first_new, second_new)


def on_device(
    tokens,
    cotangent,
    counts,
    qkv_weight,
    proj_weight,
    expand_weight,
    reduce_weight,
    qv_bias,
    expand_bias,
    vectors,
    first_qkv_weight,
    second_qkv_weight,
    first_proj_weight,
    second_proj_weight,
    first_expand_weight,
    second_expand_weight,
    first_reduce_weight,
    second_reduce_weight,
    first_qv_bias,
    second_qv_bias,
    first_expand_bias,
    second_expand_bias,
    first_vectors,
    second_vectors,
):
    n_dp = lax.axis_size("dp")
    n_t = lax.axis_size("tensor")
    slots, seq, width = tokens.shape
    n_img = slots // n_t
    rows = -(-seq // 16) * 16
    own_d = qkv_weight.shape[0]
    q_width = qkv_weight.shape[2]
    n_heads = q_width // HEAD_DIM
    ff = expand_weight.shape[1]
    qb, eb, vb = qv_bias.shape[1], expand_bias.shape[0], vectors.shape[1]
    wide = -(-3 * q_width // 128) * 128
    pad = wide - 3 * q_width

    shard_q = jnp.concatenate(
        [qkv_weight.reshape(own_d, 3 * q_width), proj_weight.T], axis=1
    ).astype(bf16)
    shard_e = expand_weight.astype(bf16)
    shard_r = reduce_weight.T.astype(bf16)
    n_small = 2 * qb + eb + 6 * vb
    small = jnp.concatenate(
        [qv_bias.reshape(-1), expand_bias, vectors.reshape(-1), jnp.zeros((width - n_small,), f32)]
    )
    shard_s = jnp.zeros((SMALL_ROWS, width), bf16).at[0].set(small.astype(bf16))
    g_s, g_q, g_e, g_r = gather_all([shard_s, shard_q, shard_e, shard_r], n_dp)
    w_q = g_q.reshape(n_t, width, width)
    w_e = g_e.reshape(n_t, width, ff)
    w_r = g_r.reshape(n_t, width, ff)
    got_s = g_s.reshape(n_t, n_dp, SMALL_ROWS, width)[:, :, 0].astype(f32)
    b_qv = got_s[:, :, : 2 * qb].reshape(n_t, n_dp, 2, qb).transpose(0, 2, 1, 3).reshape(n_t, 2, q_width)
    b_exp = got_s[:, :, 2 * qb : 2 * qb + eb].reshape(n_t, 1, ff)
    vec = got_s[0, :, 2 * qb + eb : n_small].reshape(n_dp, 6, vb).transpose(1, 0, 2).reshape(6, width)
    vec = jnp.pad(vec, ((0, 2), (0, 0)))
    bias = jnp.concatenate(
        [b_qv[:, 0], jnp.zeros((n_t, q_width), f32), b_qv[:, 1], jnp.zeros((n_t, pad), f32)], axis=1
    )
    bias = jnp.pad(bias[:, None], ((0, 0), (0, 7), (0, 0)))
    b_exp = jnp.pad(b_exp, ((0, 0), (0, 7), (0, 0)))

    start = lax.axis_index("tensor") * n_img
    where = jnp.stack([start, counts[0]]).astype(jnp.int32)
    a1, qkv, mixp, lse = front(where, tokens, vec, bias, w_q, n_img, rows, n_heads)
    a2, hid, dpre, gh, dres, drh, dmix, out_t, dvec_a, dbexp = middle(
        where, tokens, cotangent, mixp, vec, b_exp, w_q, w_e, w_r, n_img, rows
    )
    dqkv, gt_t, dvec_b, dbias = back(where, tokens, qkv, lse, dmix, dres, vec, w_q, n_img, rows, n_heads)

    output = lax.all_to_all(out_t, "tensor", 0, 0, tiled=True).astype(f32).reshape(slots, seq, -1)
    grad_tokens = lax.all_to_all(gt_t, "tensor", 0, 0, tiled=True).astype(f32).reshape(slots, seq, -1)

    d_r = dot_tn(gh, hid).astype(bf16)
    d_e = dot_tn(a2, dpre).astype(bf16)
    mix = mixp.shape[1] // n_t
    d_q = dot_tn(a1, dqkv).reshape(width, n_t, wide)
    d_p = dot_tn(drh, mixp).reshape(width, n_t, mix)
    d_q = (
        (
            jnp.pad(d_q, ((0, 0), (0, 0), (0, width - wide)))
            + jnp.pad(d_p, ((0, 0), (0, 0), (width - mix, 0)))
        )
        .astype(bf16)
        .reshape(width, n_t * width)
    )
    dvec = jnp.concatenate([dvec_b[0:2], dvec_a[2:6]], axis=0)
    db = dbias[:, 0]
    s_qv = jnp.stack([db[:, :q_width], db[:, 2 * q_width : 3 * q_width]], axis=1)
    s_qv = s_qv.reshape(n_t, 2, n_dp, qb).transpose(2, 0, 1, 3).reshape(n_dp, n_t, 2 * qb)
    s_exp = dbexp[:, 0].reshape(n_t, n_dp, eb).transpose(1, 0, 2)
    s_vec = dvec.reshape(6, n_dp, vb).transpose(1, 0, 2).reshape(n_dp, 1, 6 * vb)
    s_vec = jnp.broadcast_to(s_vec, (n_dp, n_t, 6 * vb))
    d_s = jnp.concatenate([s_qv, s_exp, s_vec, jnp.zeros((n_dp, n_t, width - n_small), f32)], axis=2)
    d_s = jnp.pad(d_s.reshape(n_dp, 1, n_t * width), ((0, 0), (0, SMALL_ROWS - 1), (0, 0)))
    d_s = d_s.reshape(n_dp * SMALL_ROWS, n_t * width).astype(bf16)
    g_s, g_r, g_e, g_q = reduce_all([d_s, d_r, d_e, d_q], [width, ff, ff, width], n_dp)

    g_qkv = g_q[:, : 3 * q_width].reshape(own_d, 3, q_width)
    g_proj = g_q[:, 3 * q_width :].T
    g_expand = g_e
    g_reduce = g_r.T
    g_row = g_s[0]
    g_qvb = g_row[: 2 * qb].reshape(2, qb)
    g_expb = g_row[2 * qb : 2 * qb + eb]
    g_vec = g_row[2 * qb + eb : n_small].reshape(6, vb)

    results = [output, grad_tokens]
    for master, grad, first, second, rate, wd in (
        (qkv_weight, g_qkv, first_qkv_weight, second_qkv_weight, lr_matrix, decay),
        (proj_weight, g_proj, first_proj_weight, second_proj_weight, lr_matrix, decay),
        (expand_weight, g_expand, first_expand_weight, second_expand_weight, lr_matrix, decay),
        (reduce_weight, g_reduce, first_reduce_weight, second_reduce_weight, lr_matrix, decay),
        (qv_bias, g_qvb, first_qv_bias, second_qv_bias, lr_vector, 0.0),
        (expand_bias, g_expb, first_expand_bias, second_expand_bias, lr_vector, 0.0),
        (vectors, g_vec, first_vectors, second_vectors, lr_vector, 0.0),
    ):
        results.append(grad)
        results.extend(adamw(master, grad, first, second, rate, wd))
    return tuple(results)


def solution(mesh):
    matrix = {
        "qkv": P("dp", None, "tensor"),
        "proj": P("tensor", "dp"),
        "expand": P("dp", "tensor"),
        "reduce": P("tensor", "dp"),
        "qvb": P(None, ("tensor", "dp")),
        "expb": P(("tensor", "dp")),
        "vec": P(None, "dp"),
    }
    specs = list(matrix.values())
    in_specs = [P("dp", None, None), P("dp", None, None), P("dp")] + specs
    out_specs = [P("dp", None, "tensor"), P("dp", None, "tensor")]
    for s in specs:
        in_specs += [s, s]
        out_specs += [s, s, s, s]
    return jax.shard_map(
        on_device,
        mesh=mesh,
        in_specs=tuple(in_specs),
        out_specs=tuple(out_specs),
        check_vma=False,
    )
```

```python
import functools

import jax
import jax.numpy as jnp
from jax import lax
from jax.experimental import pallas as pl
from jax.experimental.pallas import tpu as pltpu
from jax.sharding import PartitionSpec as P

HEAD_DIM = 64
f32 = jnp.float32
bf16 = jnp.bfloat16

lr_matrix = 0.006
lr_vector = 0.1
decay = 0.05
beta_one = 0.9
beta_two = 0.999
adam_eps = 1e-08
adam_step = 2.0
norm_eps = 1e-06
SMALL_ROWS = 16
VMEM_MAX = 63 * 1024 * 1024


def dot_nn(a, b):
    return lax.dot_general(a, b, (((1,), (0,)), ((), ())), preferred_element_type=f32)


def dot_nt(a, b):
    return lax.dot_general(a, b, (((1,), (1,)), ((), ())), preferred_element_type=f32)


def dot_tn(a, b):
    return lax.dot_general(a, b, (((0,), (0,)), ((), ())), preferred_element_type=f32)


def half_round(v):
    return v.astype(bf16).astype(f32)


def norm_stats(rows):
    mean = jnp.mean(rows, axis=-1, keepdims=True)
    centred = rows - mean
    variance = jnp.mean(centred * centred, axis=-1, keepdims=True)
    scale = lax.rsqrt(variance + norm_eps)
    return centred * scale, scale


def norm_back(grad_in, normed, scale, gain):
    scaled = grad_in * gain
    return scale * (
        scaled
        - jnp.mean(scaled, axis=-1, keepdims=True)
        - normed * jnp.mean(scaled * normed, axis=-1, keepdims=True)
    )


def places(n_z):
    dp = lax.axis_index("dp")
    t = lax.axis_index("tensor")
    z, x = dp // 2, dp % 2
    y, c = t // 2, t % 2
    fy, fx = 1 - 2 * y, 1 - 2 * x
    first = (dp + c * fx, t + (1 - c) * 2 * fy)
    second = (dp + (1 - c) * fx, t + c * 2 * fy)
    sibling = (dp, t + 1 - 2 * c)
    sets = (
        (y, x),
        (y + (1 - c) * fy, x + c * fx),
        (y + c * fy, x + (1 - c) * fx),
        (1 - y, 1 - x),
    )
    along_z = [(lax.rem(z + k, n_z) * 2 + x, t) for k in range(1, n_z)]
    return z, x, y, c, first, second, sibling, sets, along_z


def greet(peers):
    barrier = pltpu.get_barrier_semaphore()
    for peer in peers:
        pl.semaphore_signal(barrier, inc=1, device_id=peer, device_id_type=pl.DeviceIdType.MESH)
    pl.semaphore_wait(barrier, len(peers))


def push(src, dst, send, recv, peer):
    return pltpu.make_async_remote_copy(
        src_ref=src,
        dst_ref=dst,
        send_sem=send,
        recv_sem=recv,
        device_id=peer,
        device_id_type=pl.DeviceIdType.MESH,
    )


def gather_body(n_w, n_z, *refs):
    shards, outs = refs[:n_w], refs[n_w : 2 * n_w]
    local_sem, z_send, z_recv, s_send, s_recv = refs[2 * n_w :]
    z, x, y, c, first, second, sibling, sets, along_z = places(n_z)
    greet([first, second, sibling] + along_z)

    def own(w):
        return pltpu.make_async_copy(shards[w], outs[w].at[y, c, z, x], local_sem.at[w])

    def to_z(w, k):
        return push(shards[w], outs[w].at[y, c, z, x], z_send.at[w, k], z_recv.at[w, k], along_z[k])

    def move(w, which, peer, slot):
        sy, sx = sets[which]
        part = outs[w].at[sy, c, :, sx]
        return push(part, part, s_send.at[w, slot], s_recv.at[w, slot], peer)

    plan = {
        0: (0, first),
        1: (0, second),
        2: (1, second),
        3: (0, sibling),
        4: (1, sibling),
        5: (2, sibling),
        6: (3, sibling),
    }

    def go(w, slot):
        which, peer = plan[slot]
        move(w, which, peer, slot).start()

    def arrived(w, slot):
        which, peer = plan[slot]
        move(w, which, peer, slot).wait_recv()

    for w in range(n_w):
        own(w).start()
        for k in range(n_z - 1):
            to_z(w, k).start()
    for step in range(n_w + 3):
        w = step
        if 0 <= w < n_w:
            own(w).wait()
            for k in range(n_z - 1):
                to_z(w, k).wait_recv()
            for slot in (0, 1, 3):
                go(w, slot)
        w = step - 1
        if 0 <= w < n_w:
            arrived(w, 0)
            go(w, 2)
            go(w, 4)
        w = step - 2
        if 0 <= w < n_w:
            arrived(w, 1)
            go(w, 5)
            arrived(w, 2)
            go(w, 6)
        w = step - 3
        if 0 <= w < n_w:
            for slot in (3, 4, 5, 6):
                arrived(w, slot)
    for w in range(n_w):
        for k in range(n_z - 1):
            to_z(w, k).wait_send()
        for slot, (which, peer) in plan.items():
            move(w, which, peer, slot).wait_send()


def gather_all(shards, n_dp):
    n_w, n_z = len(shards), n_dp // 2
    shapes = [(2, 2, n_z, 2) + s.shape for s in shards]
    return pl.pallas_call(
        functools.partial(gather_body, n_w, n_z),
        out_shape=[jax.ShapeDtypeStruct(s, bf16) for s in shapes],
        in_specs=[pl.BlockSpec(memory_space=pltpu.VMEM)] * n_w,
        out_specs=[pl.BlockSpec(memory_space=pl.ANY)] * n_w,
        scratch_shapes=[
            pltpu.SemaphoreType.DMA((n_w,)),
            pltpu.SemaphoreType.DMA((n_w, n_z - 1)),
            pltpu.SemaphoreType.DMA((n_w, n_z - 1)),
            pltpu.SemaphoreType.DMA((n_w, 7)),
            pltpu.SemaphoreType.DMA((n_w, 7)),
        ],
        compiler_params=pltpu.CompilerParams(collective_id=0, has_side_effects=True),
        name="gather_weights",
    )(*shards)


def key_mask(rows, seq):
    return lax.broadcasted_iota(jnp.int32, (rows, rows), 1) < seq


def load_rows(src, dst, seq):
    dst[pl.ds(0, seq), :] = src[0]


def front_body(seq, n_heads, where, x_ref, vec_ref, bias_ref, wq_ref, a1_ref, n1_ref, qkv_ref, mix_ref, lse_ref, xs):
    rows = xs.shape[0]

    @pl.when(pl.program_id(0) == 0)
    def _():
        xs[...] = jnp.zeros_like(xs)

    load_rows(x_ref, xs, seq)
    normed, scale = norm_stats(xs[...])
    n1_ref[...] = normed
    a1 = (normed * vec_ref[0:1, :] + vec_ref[1:2, :]).astype(bf16)
    a1_ref[...] = a1
    mask = key_mask(rows, seq)
    lane = lax.broadcasted_iota(jnp.int32, (rows, 128), 1)
    lse_ref[...] = jnp.where(lane == 127, scale, 0.0)
    q_width = n_heads * HEAD_DIM
    wide = bias_ref.shape[2]
    pad = mix_ref.shape[1] // 4 - q_width
    for t in range(4):
        qkv = (dot_nn(a1_ref[...], wq_ref[t, :, :wide]) + bias_ref[t, 0:1, :]).astype(bf16)
        qkv_ref[:, t * wide : (t + 1) * wide] = qkv
        outs = [jnp.zeros((rows, pad), bf16)]
        for h in range(n_heads):
            q = qkv[:, h * HEAD_DIM : (h + 1) * HEAD_DIM]
            k = qkv[:, q_width + h * HEAD_DIM : q_width + (h + 1) * HEAD_DIM]
            v = qkv[:, 2 * q_width + h * HEAD_DIM : 2 * q_width + (h + 1) * HEAD_DIM]
            s = jnp.where(mask, dot_nt(q, k) * (HEAD_DIM**-0.5), -1e30)
            top = jnp.max(s, axis=-1, keepdims=True)
            e = jnp.exp(s - top)
            total = jnp.sum(e, axis=-1, keepdims=True)
            p = (e * (1.0 / total)).astype(bf16)
            outs.append(dot_nn(p, v).astype(bf16))
            lse = top + jnp.log(total)
            lse_ref[...] = jnp.where(lane == t * n_heads + h, lse, lse_ref[...])
        mix_ref[:, t * (pad + q_width) : (t + 1) * (pad + q_width)] = jnp.concatenate(outs, axis=1)


def front(where, tokens, vec, bias, wq, n_img, rows, n_heads):
    slots, seq, width = tokens.shape
    wide = bias.shape[2]
    mix = width - (3 * n_heads * HEAD_DIM // 128) * 128
    total = n_img * rows
    return pl.pallas_call(
        functools.partial(front_body, seq, n_heads),
        out_shape=[
            jax.ShapeDtypeStruct((total, width), bf16),
            jax.ShapeDtypeStruct((total, width), f32),
            jax.ShapeDtypeStruct((total, 4 * wide), bf16),
            jax.ShapeDtypeStruct((total, 4 * mix), bf16),
            jax.ShapeDtypeStruct((total, 128), f32),
        ],
        grid_spec=pltpu.PrefetchScalarGridSpec(
            num_scalar_prefetch=1,
            grid=(n_img,),
            in_specs=[
                pl.BlockSpec((1, seq, width), lambda i, s: (s[0] + i, 0, 0)),
                pl.BlockSpec(vec.shape, lambda i, s: (0, 0)),
                pl.BlockSpec(bias.shape, lambda i, s: (0, 0, 0)),
                pl.BlockSpec(wq.shape, lambda i, s: (0, 0, 0), pipeline_mode=pl.Buffered(1)),
            ],
            out_specs=[
                pl.BlockSpec((rows, width), lambda i, s: (i, 0)),
                pl.BlockSpec((rows, width), lambda i, s: (i, 0)),
                pl.BlockSpec((rows, 4 * wide), lambda i, s: (i, 0)),
                pl.BlockSpec((rows, 4 * mix), lambda i, s: (i, 0)),
                pl.BlockSpec((rows, 128), lambda i, s: (i, 0)),
            ],
            scratch_shapes=[pltpu.VMEM((rows, width), f32)],
        ),
        compiler_params=pltpu.CompilerParams(vmem_limit_bytes=VMEM_MAX),
        name="front",
    )(where, tokens, vec, bias, wq)


def middle_body(
    seq,
    where,
    x_ref,
    cot_ref,
    mix_ref,
    vec_ref,
    bexp_ref,
    wq_ref,
    we_ref,
    wr_ref,
    a2_ref,
    hd_ref,
    gh_ref,
    dres_ref,
    drh_ref,
    dmix_ref,
    out_ref,
    dvec_ref,
    dbexp_ref,
    xs,
    gs,
):
    i = pl.program_id(0)

    @pl.when(i == 0)
    def _():
        xs[...] = jnp.zeros_like(xs)
        gs[...] = jnp.zeros_like(gs)
        dvec_ref[...] = jnp.zeros_like(dvec_ref)
        dbexp_ref[...] = jnp.zeros_like(dbexp_ref)

    live = jnp.where(where[0] + i < where[1], 1.0, 0.0).astype(f32)
    load_rows(x_ref, xs, seq)
    gs[pl.ds(0, seq), :] = cot_ref[0] * live
    rows, width = xs.shape
    mix = mix_ref.shape[1] // 4
    ff = we_ref.shape[2]
    att = jnp.zeros((rows, width), f32)
    for t in range(4):
        att += half_round(dot_nt(mix_ref[:, t * mix : (t + 1) * mix], wq_ref[t, :, width - mix :]))
    resid = xs[...] + att + vec_ref[2:3, :]
    normed2, scale2 = norm_stats(resid)
    a2_ref[...] = (normed2 * vec_ref[3:4, :] + vec_ref[4:5, :]).astype(bf16)
    gh_ref[...] = gs[...].astype(bf16)
    feed = jnp.zeros((rows, width), f32)
    d_a2 = jnp.zeros((rows, width), f32)
    for t in range(4):
        pre = dot_nn(a2_ref[...], we_ref[t]) + bexp_ref[t, 0:1, :]
        cdf = 0.5 + 0.5 * lax.erf(pre * (0.5**0.5))
        hid = (pre * cdf).astype(bf16)
        slope = cdf + pre * jnp.exp(-0.5 * pre * pre) * ((2.0 * jnp.pi) ** -0.5)
        hd_ref[:, t * ff : (t + 1) * ff] = hid
        d_pre = dot_nn(gh_ref[...], wr_ref[t]) * slope
        dbexp_ref[t, 0:1, :] += jnp.sum(d_pre, axis=0, keepdims=True)
        dph = d_pre.astype(bf16)
        hd_ref[:, (4 + t) * ff : (5 + t) * ff] = dph
        feed += half_round(dot_nt(hid, wr_ref[t]))
        d_a2 += half_round(dot_nt(dph, we_ref[t]))
    out = (resid + feed + vec_ref[5:6, :]) * live
    col = width // 2
    for t in range(2):
        out_ref[t, 0] = out[:seq, t * col : (t + 1) * col].astype(bf16)
    d_resid = gs[...] + norm_back(d_a2, normed2, scale2, vec_ref[3:4, :])
    dres_ref[...] = d_resid
    drh = d_resid.astype(bf16)
    drh_ref[...] = drh
    for t in range(4):
        dmix_ref[:, t * mix : (t + 1) * mix] = dot_nn(drh, wq_ref[t, :, width - mix :]).astype(bf16)
    dvec_ref[2:3, :] += jnp.sum(d_resid, axis=0, keepdims=True)
    dvec_ref[3:4, :] += jnp.sum(d_a2 * normed2, axis=0, keepdims=True)
    dvec_ref[4:5, :] += jnp.sum(d_a2, axis=0, keepdims=True)
    dvec_ref[5:6, :] += jnp.sum(gs[...], axis=0, keepdims=True)


def middle(where, tokens, cotangent, mixp, vec, bexp, wq, we, wr, n_img, rows):
    slots, seq, width = tokens.shape
    ff = we.shape[2]
    mix = mixp.shape[1]
    total = n_img * rows
    col = width // 2
    row_block = lambda n: pl.BlockSpec((rows, n), lambda i, s: (i, 0))
    whole = lambda a: pl.BlockSpec(
        a.shape, lambda i, s, nd=len(a.shape): (0,) * nd, pipeline_mode=pl.Buffered(1)
    )
    image = pl.BlockSpec((1, seq, width), lambda i, s: (s[0] + i, 0, 0))
    return pl.pallas_call(
        functools.partial(middle_body, seq),
        out_shape=[
            jax.ShapeDtypeStruct((total, width), bf16),
            jax.ShapeDtypeStruct((total, 8 * ff), bf16),
            jax.ShapeDtypeStruct((total, width), bf16),
            jax.ShapeDtypeStruct((total, width), f32),
            jax.ShapeDtypeStruct((total, width), bf16),
            jax.ShapeDtypeStruct((total, mix), bf16),
            jax.ShapeDtypeStruct((2, n_img, seq, col), bf16),
            jax.ShapeDtypeStruct((8, width), f32),
            jax.ShapeDtypeStruct((4, 8, ff), f32),
        ],
        grid_spec=pltpu.PrefetchScalarGridSpec(
            num_scalar_prefetch=1,
            grid=(n_img,),
            in_specs=[image, image, row_block(mix)] + [whole(a) for a in (vec, bexp, wq, we, wr)],
            out_specs=[
                row_block(width),
                row_block(8 * ff),
                row_block(width),
                row_block(width),
                row_block(width),
                row_block(mix),
                pl.BlockSpec((2, 1, seq, col), lambda i, s: (0, i, 0, 0)),
                pl.BlockSpec((8, width), lambda i, s: (0, 0)),
                pl.BlockSpec((4, 8, ff), lambda i, s: (0, 0, 0)),
            ],
            scratch_shapes=[pltpu.VMEM((rows, width), f32), pltpu.VMEM((rows, width), f32)],
        ),
        compiler_params=pltpu.CompilerParams(vmem_limit_bytes=VMEM_MAX),
        name="middle",
    )(where, tokens, cotangent, mixp, vec, bexp, wq, we, wr)


S_ROWS = 24


def attention_back(seq, n_heads, qkv_ref, lse_ref, dmix_ref, t, wide, mix):
    rows = qkv_ref.shape[0]
    q_width = n_heads * HEAD_DIM
    scale_qk = HEAD_DIM**-0.5
    mask = key_mask(rows, seq)
    dq, dk, dv = [], [], []
    for h in range(n_heads):
        at = t * wide + h * HEAD_DIM
        q = qkv_ref[:, at : at + HEAD_DIM]
        k = qkv_ref[:, at + q_width : at + q_width + HEAD_DIM]
        v = qkv_ref[:, at + 2 * q_width : at + 2 * q_width + HEAD_DIM]
        m_at = (t + 1) * mix - q_width + h * HEAD_DIM
        dm = dmix_ref[:, m_at : m_at + HEAD_DIM]
        lse = lse_ref[:, t * n_heads + h : t * n_heads + h + 1]
        p = jnp.where(mask, jnp.exp(dot_nt(q, k) * scale_qk - lse), 0.0)
        dv.append(dot_tn(p.astype(bf16), dm))
        d_p = dot_nt(dm, v)
        delta = jnp.sum(p * d_p, axis=-1, keepdims=True)
        ds = (p * (d_p - delta) * scale_qk).astype(bf16)
        dq.append(dot_nn(ds, k))
        dk.append(dot_tn(ds, q))
    return jnp.concatenate(dq + dk + dv + [jnp.zeros((rows, wide - 3 * q_width), f32)], axis=1)


def rear_body(cfg, *refs):
    n_z, n_img, seq, rows, n_heads, shard_rows, wide, mix, ff = cfg
    (hd_ref, mix_ref, qkv_ref, lse_ref, dmix_ref, dres_ref, n1_ref, vec_ref, wq_ref, dvec_in, dbexp_in) = refs[:11]
    gh_any, a2_any, a1_any, drh_any, out2_any = refs[11:16]
    gr_out, ge_out, gq_out, gs_out, ro_out, rg_out = refs[16:22]
    (lhs_a, lhs_b, dqs, gts) = refs[22:26]
    part, got, got2, got1, gotz = (refs[26 + 3 * k : 29 + 3 * k] for k in range(5))
    sv, sgot, sz = refs[41:44]
    (
        lhs_sem,
        load_sem,
        keep_sem,
        o_send,
        o_recv,
        g_send,
        g_recv,
        f_send,
        f_recv,
        h_send,
        h_recv,
        s_send,
        s_recv,
        z_send,
        z_recv,
        v_send,
        v_recv,
        vz_send,
        vz_recv,
    ) = refs[44:]
    outs = (gr_out, ge_out, gq_out)
    s = pl.program_id(0)
    n_t = 4
    base_e, base_b = n_t, 2 * n_t
    base_q = base_b + n_img
    base_t = base_q + n_t
    width = n1_ref.shape[1]
    n_dp = 2 * n_z

    dp = lax.axis_index("dp")
    t_me = lax.axis_index("tensor")
    z, x = dp // 2, dp % 2
    y, c = t_me // 2, t_me % 2
    fy, fx = 1 - 2 * y, 1 - 2 * x
    sibling = (dp, t_me + 1 - 2 * c)
    over_y = (dp, t_me + 2 * fy)
    over_x = (dp + fx, t_me)
    along_z = [(lax.rem(z + k, n_z) * 2 + x, t_me) for k in range(1, n_z)]

    def route(w):
        m = c if w == 2 else 0 * c
        first = (dp + m * fx, t_me + (1 - m) * 2 * fy)
        second = (dp + (1 - m) * fx, t_me + m * 2 * fy)
        sets = (
            (y, x),
            (y + (1 - m) * fy, x + m * fx),
            (y + m * fy, x + (1 - m) * fx),
            (1 - y, 1 - x),
        )
        return first, second, sets

    def half(w, yy):
        return push(part[w].at[1 - c, yy], got[w].at[yy], h_send.at[w, yy], h_recv.at[w, yy], sibling)

    def to_second(w, k):
        first, second, sets = route(w)
        sy, sx = sets[k]
        return push(
            part[w].at[c, sy, sx], got2[w].at[k - 2], s_send.at[w, k - 2], s_recv.at[w, k - 2], second
        )

    def to_first(w):
        first, second, sets = route(w)
        sy, sx = sets[1]
        return push(part[w].at[c, sy, sx], got1[w], s_send.at[w, 2], s_recv.at[w, 2], first)

    def to_z(w, k):
        return push(
            part[w].at[c, y, x, along_z[k][0] // 2],
            gotz[w].at[k],
            z_send.at[w, k],
            z_recv.at[w, k],
            along_z[k],
        )

    def add(w, k, other):
        sy, sx = route(w)[2][k]

        def one(i, carry):
            mine = part[w][c, sy, sx, i].astype(f32)
            part[w][c, sy, sx, i] = (mine + other(sy, sx, i).astype(f32)).astype(bf16)
            return carry

        lax.fori_loop(0, n_z, one, 0)

    def stage_b(w):
        half(w, 0).wait_recv()
        half(w, 1).wait_recv()
        for k in (3, 2, 1, 0):
            add(w, k, lambda sy, sx, i: got[w][sy, sx, i])
            if k >= 2:
                to_second(w, k).start()

    def stage_c(w):
        to_second(w, 3).wait_recv()
        add(w, 1, lambda sy, sx, i: got2[w][1, i])
        to_first(w).start()
        to_second(w, 2).wait_recv()
        add(w, 0, lambda sy, sx, i: got2[w][0, i])

    def stage_d(w):
        to_first(w).wait_recv()
        add(w, 0, lambda sy, sx, i: got1[w][i])
        for k in range(n_z - 1):
            to_z(w, k).start()

    def stage_f(w):
        total = part[w][c, y, x, z].astype(f32)
        for k in range(n_z - 1):
            to_z(w, k).wait_recv()
            total = total + gotz[w][k].astype(f32)
        outs[w][...] = total

    def small(k):
        peer = (sibling, over_x, over_y)[k]
        return push(sv.at[k], sgot.at[k], v_send.at[k], v_recv.at[k], peer)

    def small_step(k):
        small(k).wait_recv()
        sv[k + 1] = sv[k] + sgot[k]
        if k < 2:
            small(k + 1).start()
        else:
            sz[z] = sv[3]
            for j in range(n_z - 1):
                small_z(j).start()

    def small_z(j):
        return push(sv.at[3], sz.at[z], vz_send.at[j], vz_recv.at[j], along_z[j])

    def small_end():
        for j in range(n_z - 1):
            small_z(j).wait_recv()
        total = sz[0]
        for j in range(1, n_z):
            total = total + sz[j]
        gs_out[...] = total

    def load(k, src):
        return pltpu.make_async_copy(src, (lhs_a, lhs_b)[k], lhs_sem.at[k])

    def out_load():
        return pltpu.make_async_copy(out2_any, gts, load_sem.at[0])

    def out_keep():
        return pltpu.make_async_copy(gts.at[y], ro_out.at[t_me], keep_sem.at[0])

    def out_sibling():
        return push(out2_any.at[y], ro_out.at[t_me], o_send.at[0], o_recv.at[0], sibling)

    def out_y():
        return push(out2_any.at[1 - y], ro_out.at[t_me], o_send.at[1], o_recv.at[1], over_y)

    def forward(ref, slot):
        row = ref.at[t_me + 2 * fy]
        return push(row, row, f_send.at[slot], f_recv.at[slot], sibling)

    def gt_keep(i):
        return pltpu.make_async_copy(gts.at[y, i], rg_out.at[t_me, i], keep_sem.at[1 + i])

    def gt_sibling(i):
        return push(gts.at[y, i], rg_out.at[t_me, i], g_send.at[i, 0], g_recv.at[i, 0], sibling)

    def gt_y(i):
        return push(gts.at[1 - y, i], rg_out.at[t_me, i], g_send.at[i, 1], g_recv.at[i, 1], over_y)

    def at(step):
        return pl.when(s == step)

    @at(0)
    def _():
        load(0, gh_any).start()
        load(1, a2_any).start()
        out_load().start()
        greet([sibling, over_x, over_y] + along_z)
        out_y().start()
        out_sibling().start()
        sv[...] = jnp.zeros_like(sv)
        load(0, gh_any).wait()
        load(1, a2_any).wait()
        out_load().wait()
        out_keep().start()

    @at(base_e + 1)
    def _():
        stage_b(0)

    @at(base_b)
    def _():
        load(0, a1_any).start()
        load(1, drh_any).start()
        out_keep().wait()
        out_y().wait_recv()
        forward(ro_out, 0).start()

    early = [
        (base_b + 1, lambda: stage_b(1)),
        (base_b + 2, lambda: stage_c(0)),
        (base_b + 3, lambda: stage_d(0)),
        (base_b + 4, lambda: stage_c(1)),
        (base_b + 4, lambda: stage_f(0)),
    ]
    for step, event in early:
        at(min(step, base_q))(event)

    @at(base_q)
    def _():
        stage_d(1)
        load(0, a1_any).wait()
        load(1, drh_any).wait()
        small(0).start()

    at(base_q + 1)(lambda: small_step(0))
    at(base_q + 2)(lambda: small_step(1))

    @at(base_q + 3)
    def _():
        stage_f(1)
        small_step(2)

    @at(base_t)
    def _():
        stage_b(2)
        small_end()
        for i in range(n_img):
            gt_y(i).wait_recv()
        forward(rg_out, 1).start()

    at(base_t + 1)(lambda: stage_c(2))
    at(base_t + 2)(lambda: stage_d(2))

    def put(w, t, g):
        g = g.astype(bf16)
        for d in range(n_dp):
            part[w][t % 2, t // 2, d % 2, d // 2] = g[d * shard_rows : (d + 1) * shard_rows]

    @pl.when(s < base_e)
    def _():
        put(0, s, dot_tn(lhs_a[...], hd_ref[...]))

    @pl.when((s >= base_e) & (s < base_b))
    def _():
        put(1, s - base_e, dot_tn(lhs_b[...], hd_ref[...]))

    @pl.when((s >= base_b) & (s < base_q))
    def _():
        i = s - base_b
        d_a1 = jnp.zeros((rows, width), f32)
        for t in range(4):
            d_all = attention_back(seq, n_heads, qkv_ref, lse_ref, dmix_ref, t, wide, mix)
            sv[0, 4 + t : 5 + t, :wide] += jnp.sum(d_all, axis=0, keepdims=True)
            d_half = d_all.astype(bf16)
            dqs[t, pl.ds(i * rows, rows), :] = d_half
            d_a1 += half_round(dot_nt(d_half, wq_ref[t, :, :wide]))
        normed, scale = n1_ref[...], lse_ref[:, 127:128]
        grad = dres_ref[...] + norm_back(d_a1, normed, scale, vec_ref[0:1, :])
        col = width // 2
        for h in range(2):
            gts[h, i] = grad[:seq, h * col : (h + 1) * col].astype(bf16)
        sv[0, 8:9, :] += jnp.sum(d_a1 * normed, axis=0, keepdims=True)
        sv[0, 9:10, :] += jnp.sum(d_a1, axis=0, keepdims=True)

    @pl.when((s >= base_q) & (s < base_t))
    def _():
        t = s - base_q
        dq = dot_tn(lhs_a[...], dqs[t])
        dp_ = dot_tn(lhs_b[...], mix_ref[...])
        cut = width - mix
        put(
            2,
            t,
            jnp.concatenate(
                [dq[:, :cut], dq[:, cut:] + dp_[:, : wide - cut], dp_[:, wide - cut :]], axis=1
            ),
        )

    at(1)(lambda: half(0, 0).start())
    at(3)(lambda: half(0, 1).start())
    at(base_e + 1)(lambda: half(1, 0).start())
    at(base_e + 3)(lambda: half(1, 1).start())
    for i in range(n_img):

        @at(base_b + i)
        def _(i=i):
            gt_keep(i).start()
            gt_y(i).start()
            gt_sibling(i).start()

    @at(base_q - 1)
    def _():
        sv[0, 10:14, :] = dvec_in[2:6, :]
        for t in range(4):
            sv[0, t : t + 1, :] = dbexp_in[t, 0:1, :]

    at(base_q + 1)(lambda: half(2, 0).start())
    at(base_q + 3)(lambda: half(2, 1).start())

    @at(base_t + 3)
    def _():
        stage_f(2)
        out_sibling().wait_recv()
        forward(ro_out, 0).wait_recv()
        for i in range(n_img):
            gt_keep(i).wait()
            gt_sibling(i).wait_recv()
        forward(rg_out, 1).wait_recv()
        out_sibling().wait_send()
        out_y().wait_send()
        for i in range(n_img):
            gt_sibling(i).wait_send()
            gt_y(i).wait_send()
        forward(ro_out, 0).wait_send()
        forward(rg_out, 1).wait_send()
        for w in range(3):
            half(w, 0).wait_send()
            half(w, 1).wait_send()
            to_second(w, 2).wait_send()
            to_second(w, 3).wait_send()
            to_first(w).wait_send()
            for k in range(n_z - 1):
                to_z(w, k).wait_send()
        for k in range(3):
            small(k).wait_send()
        for j in range(n_z - 1):
            small_z(j).wait_send()


def rear(hd, mixp, qkv, lse, dmix, dres, n1, vec, wq, dvec, dbexp, gh, a2, a1, drh, out2, n_dp, n_img, n_heads):
    total, width = n1.shape
    rows = total // n_img
    ff = hd.shape[1] // 8
    wide, mix = qkv.shape[1] // 4, mixp.shape[1] // 4
    seq, col = out2.shape[2], out2.shape[3]
    n_z = n_dp // 2
    shard_rows = width // n_dp
    n_t = 4
    base_b = 2 * n_t
    base_q = base_b + n_img
    n_steps = base_q + n_t + 4
    cfg = (n_z, n_img, seq, rows, n_heads, shard_rows, wide, mix, ff)
    image = lambda s: (jnp.clip(s - base_b, 0, n_img - 1), 0)
    by_image = lambda n: pl.BlockSpec((rows, n), image)
    whole = lambda a: pl.BlockSpec(
        a.shape, lambda s, nd=len(a.shape): (0,) * nd, pipeline_mode=pl.Buffered(1)
    )
    anywhere = pl.BlockSpec(memory_space=pl.ANY)
    resident = lambda shape: pl.BlockSpec(
        shape, lambda s, nd=len(shape): (0,) * nd, pipeline_mode=pl.Buffered(1)
    )
    block = (shard_rows, width)
    dma = pltpu.SemaphoreType.DMA
    scratch = [
        pltpu.VMEM((total, width), bf16),
        pltpu.VMEM((total, width), bf16),
        pltpu.VMEM((4, total, wide), bf16),
        pltpu.VMEM((2, n_img, seq, col), bf16),
    ]
    scratch += [pltpu.VMEM((2, 2, 2, n_z) + block, bf16)] * 3
    scratch += [pltpu.VMEM((2, 2, n_z) + block, bf16)] * 3
    scratch += [pltpu.VMEM((2, n_z) + block, bf16)] * 3
    scratch += [pltpu.VMEM((n_z,) + block, bf16)] * 3
    scratch += [pltpu.VMEM((n_z - 1,) + block, bf16)] * 3
    scratch += [
        pltpu.VMEM((4, S_ROWS, width), f32),
        pltpu.VMEM((3, S_ROWS, width), f32),
        pltpu.VMEM((n_z, S_ROWS, width), f32),
    ]
    scratch += [dma((2,)), dma((1,)), dma((1 + n_img,))]
    scratch += [dma((2,))] * 2 + [dma((n_img, 2))] * 2 + [dma((2,))] * 2
    scratch += [dma((3, 2))] * 2 + [dma((3, 3))] * 2 + [dma((3, n_z - 1))] * 2
    scratch += [dma((3,))] * 2 + [dma((n_z - 1,))] * 2
    return pl.pallas_call(
        functools.partial(rear_body, cfg),
        out_shape=[jax.ShapeDtypeStruct(block, f32)] * 3
        + [jax.ShapeDtypeStruct((S_ROWS, width), f32)]
        + [jax.ShapeDtypeStruct((n_t, n_img, seq, col), bf16)] * 2,
        grid=(n_steps,),
        in_specs=[
            pl.BlockSpec((total, ff), lambda s: (0, jnp.clip(s, 0, 2 * n_t - 1))),
            pl.BlockSpec((total, mix), lambda s: (0, jnp.clip(s - base_q, 0, n_t - 1))),
            by_image(4 * wide),
            by_image(128),
            by_image(4 * mix),
            by_image(width),
            by_image(width),
            whole(vec),
            whole(wq),
            whole(dvec),
            whole(dbexp),
        ]
        + [anywhere] * 5,
        out_specs=[resident(block)] * 3 + [resident((S_ROWS, width))] + [anywhere] * 2,
        scratch_shapes=scratch,
        compiler_params=pltpu.CompilerParams(
            collective_id=1, has_side_effects=True, vmem_limit_bytes=VMEM_MAX
        ),
        name="rear",
    )(hd, mixp, qkv, lse, dmix, dres, n1, vec, wq, dvec, dbexp, gh, a2, a1, drh, out2)


def adamw(master, grad, first, second, rate, decay_rate):
    first_new = beta_one * first + (1.0 - beta_one) * grad
    second_new = beta_two * second + (1.0 - beta_two) * grad * grad
    first_hat = first_new / (1.0 - beta_one**adam_step)
    second_hat = second_new / (1.0 - beta_two**adam_step)
    new = master - rate * (first_hat / (jnp.sqrt(second_hat) + adam_eps) + decay_rate * master)
    return (new, first_new, second_new)


def on_device(
    tokens,
    cotangent,
    counts,
    qkv_weight,
    proj_weight,
    expand_weight,
    reduce_weight,
    qv_bias,
    expand_bias,
    vectors,
    first_qkv_weight,
    second_qkv_weight,
    first_proj_weight,
    second_proj_weight,
    first_expand_weight,
    second_expand_weight,
    first_reduce_weight,
    second_reduce_weight,
    first_qv_bias,
    second_qv_bias,
    first_expand_bias,
    second_expand_bias,
    first_vectors,
    second_vectors,
):
    n_dp = lax.axis_size("dp")
    n_t = lax.axis_size("tensor")
    slots, seq, width = tokens.shape
    n_img = slots // n_t
    rows = -(-seq // 16) * 16
    own_d = qkv_weight.shape[0]
    q_width = qkv_weight.shape[2]
    n_heads = q_width // HEAD_DIM
    ff = expand_weight.shape[1]
    qb, eb, vb = qv_bias.shape[1], expand_bias.shape[0], vectors.shape[1]
    wide = -(-3 * q_width // 128) * 128
    pad = wide - 3 * q_width

    shard_q = jnp.concatenate(
        [qkv_weight.reshape(own_d, 3 * q_width), proj_weight.T], axis=1
    ).astype(bf16)
    shard_e = expand_weight.astype(bf16)
    shard_r = reduce_weight.T.astype(bf16)
    n_small = 2 * qb + eb + 6 * vb
    small = jnp.concatenate(
        [qv_bias.reshape(-1), expand_bias, vectors.reshape(-1), jnp.zeros((width - n_small,), f32)]
    )
    shard_s = jnp.zeros((SMALL_ROWS, width), bf16).at[0].set(small.astype(bf16))
    g_s, g_q, g_e, g_r = gather_all([shard_s, shard_q, shard_e, shard_r], n_dp)
    w_q = g_q.reshape(n_t, width, width)
    w_e = g_e.reshape(n_t, width, ff)
    w_r = g_r.reshape(n_t, width, ff)
    got_s = g_s.reshape(n_t, n_dp, SMALL_ROWS, width)[:, :, 0].astype(f32)
    b_qv = got_s[:, :, : 2 * qb].reshape(n_t, n_dp, 2, qb).transpose(0, 2, 1, 3).reshape(n_t, 2, q_width)
    b_exp = got_s[:, :, 2 * qb : 2 * qb + eb].reshape(n_t, 1, ff)
    vec = got_s[0, :, 2 * qb + eb : n_small].reshape(n_dp, 6, vb).transpose(1, 0, 2).reshape(6, width)
    vec = jnp.pad(vec, ((0, 2), (0, 0)))
    bias = jnp.concatenate(
        [b_qv[:, 0], jnp.zeros((n_t, q_width), f32), b_qv[:, 1], jnp.zeros((n_t, pad), f32)], axis=1
    )
    bias = jnp.pad(bias[:, None], ((0, 0), (0, 7), (0, 0)))
    b_exp = jnp.pad(b_exp, ((0, 0), (0, 7), (0, 0)))

    start = lax.axis_index("tensor") * n_img
    where = jnp.stack([start, counts[0]]).astype(jnp.int32)
    a1, n1, qkv, mixp, lse = front(where, tokens, vec, bias, w_q, n_img, rows, n_heads)
    a2, hd, gh, dres, drh, dmix, out2, dvec, dbexp = middle(
        where, tokens, cotangent, mixp, vec, b_exp, w_q, w_e, w_r, n_img, rows
    )
    g_r, g_e, g_q, g_s, got_out, got_gt = rear(
        hd, mixp, qkv, lse, dmix, dres, n1, vec, w_q, dvec, dbexp, gh, a2, a1, drh, out2, n_dp, n_img, n_heads
    )
    t_me, dp_me = lax.axis_index("tensor"), lax.axis_index("dp")

    def own_columns(both):
        picked = jnp.where(t_me % 2 == 0, both[..., :q_width], both[..., q_width:])
        return picked.astype(f32).reshape(slots, seq, q_width)

    output = own_columns(got_out)
    grad_tokens = own_columns(got_gt)

    g_qkv = jnp.stack([g_q[:, j * q_width : (j + 1) * q_width] for j in range(3)], axis=1)
    g_proj = g_q[:, 3 * q_width :].T
    g_expand = g_e
    g_reduce = g_r.T
    take = lambda row, at, n: lax.dynamic_slice(g_s, (row, at), (1, n))[0]
    g_expb = take(t_me, dp_me * eb, eb)
    g_qvb = jnp.stack([take(4 + t_me, dp_me * qb, qb), take(4 + t_me, 2 * q_width + dp_me * qb, qb)])
    g_vec = lax.dynamic_slice(g_s, (8, dp_me * vb), (6, vb))

    results = [output, grad_tokens]
    for master, grad, first, second, rate, wd in (
        (qkv_weight, g_qkv, first_qkv_weight, second_qkv_weight, lr_matrix, decay),
        (proj_weight, g_proj, first_proj_weight, second_proj_weight, lr_matrix, decay),
        (expand_weight, g_expand, first_expand_weight, second_expand_weight, lr_matrix, decay),
        (reduce_weight, g_reduce, first_reduce_weight, second_reduce_weight, lr_matrix, decay),
        (qv_bias, g_qvb, first_qv_bias, second_qv_bias, lr_vector, 0.0),
        (expand_bias, g_expb, first_expand_bias, second_expand_bias, lr_vector, 0.0),
        (vectors, g_vec, first_vectors, second_vectors, lr_vector, 0.0),
    ):
        results.append(grad)
        results.extend(adamw(master, grad, first, second, rate, wd))
    return tuple(results)


def solution(mesh):
    matrix = {
        "qkv": P("dp", None, "tensor"),
        "proj": P("tensor", "dp"),
        "expand": P("dp", "tensor"),
        "reduce": P("tensor", "dp"),
        "qvb": P(None, ("tensor", "dp")),
        "expb": P(("tensor", "dp")),
        "vec": P(None, "dp"),
    }
    specs = list(matrix.values())
    in_specs = [P("dp", None, None), P("dp", None, None), P("dp")] + specs
    out_specs = [P("dp", None, "tensor"), P("dp", None, "tensor")]
    for s in specs:
        in_specs += [s, s]
        out_specs += [s, s, s, s]
    return jax.shard_map(
        on_device,
        mesh=mesh,
        in_specs=tuple(in_specs),
        out_specs=tuple(out_specs),
        check_vma=False,
    )
```

```python
import functools

import jax
import jax.numpy as jnp
from jax import lax
from jax.experimental import pallas as pl
from jax.experimental.pallas import tpu as pltpu
from jax.sharding import PartitionSpec as P

HEAD_DIM = 64
f32 = jnp.float32
bf16 = jnp.bfloat16

lr_matrix = 0.006
lr_vector = 0.1
decay = 0.05
beta_one = 0.9
beta_two = 0.999
adam_eps = 1e-08
adam_step = 2.0
norm_eps = 1e-06
VMEM_MAX = 63 * 1024 * 1024


def dot_nn(a, b):
    return lax.dot_general(a, b, (((1,), (0,)), ((), ())), preferred_element_type=f32)


def dot_nt(a, b):
    return lax.dot_general(a, b, (((1,), (1,)), ((), ())), preferred_element_type=f32)


def dot_tn(a, b):
    return lax.dot_general(a, b, (((0,), (0,)), ((), ())), preferred_element_type=f32)


def half_round(v):
    return v.astype(bf16).astype(f32)


def norm_stats(rows):
    mean = jnp.mean(rows, axis=-1, keepdims=True)
    centred = rows - mean
    variance = jnp.mean(centred * centred, axis=-1, keepdims=True)
    scale = lax.rsqrt(variance + norm_eps)
    return centred * scale, scale


def norm_back(grad_in, normed, scale, gain):
    scaled = grad_in * gain
    return scale * (
        scaled
        - jnp.mean(scaled, axis=-1, keepdims=True)
        - normed * jnp.mean(scaled * normed, axis=-1, keepdims=True)
    )


def places(n_z):
    dp = lax.axis_index("dp")
    t = lax.axis_index("tensor")
    z, x = dp // 2, dp % 2
    y, c = t // 2, t % 2
    fy, fx = 1 - 2 * y, 1 - 2 * x
    first = (dp + c * fx, t + (1 - c) * 2 * fy)
    second = (dp + (1 - c) * fx, t + c * 2 * fy)
    sibling = (dp, t + 1 - 2 * c)
    sets = (
        (y, x),
        (y + (1 - c) * fy, x + c * fx),
        (y + c * fy, x + (1 - c) * fx),
        (1 - y, 1 - x),
    )
    along_z = [(lax.rem(z + k, n_z) * 2 + x, t) for k in range(1, n_z)]
    return z, x, y, c, first, second, sibling, sets, along_z


def greet(peers):
    barrier = pltpu.get_barrier_semaphore()
    for peer in peers:
        pl.semaphore_signal(barrier, inc=1, device_id=peer, device_id_type=pl.DeviceIdType.MESH)
    pl.semaphore_wait(barrier, len(peers))


def push(src, dst, send, recv, peer):
    return pltpu.make_async_remote_copy(
        src_ref=src,
        dst_ref=dst,
        send_sem=send,
        recv_sem=recv,
        device_id=peer,
        device_id_type=pl.DeviceIdType.MESH,
    )


def key_mask(rows, seq):
    return lax.broadcasted_iota(jnp.int32, (rows, rows), 1) < seq


def load_rows(src, dst, seq):
    dst[pl.ds(0, seq), :] = src[0]


S_ROWS = 24
NAT_ROWS = 32
NAT_VEC = 8


def fore_body(cfg, *refs):
    n_z, n_img, seq, rows, n_heads, wide, mix = cfg
    (qkv_w, proj_w, exp_w, red_w, nat_own, tokens) = refs[:6]
    (gq, ge, gr, nat_ref, a1_ref, n1_ref, qkv_ref, mix_ref, lse_ref) = refs[6:15]
    (xs, xall, sh_q, sh_e, sh_r, gs, wq) = refs[15:22]
    x_sem, w_sem, local_sem, z_send, z_recv, s_send, s_recv = refs[22:]
    s = pl.program_id(0)
    z, x, y, c, first, second, sibling, sets, along_z = places(n_z)
    t_me = lax.axis_index("tensor")
    width = xs.shape[1]
    half = width // 2
    q_width = n_heads * HEAD_DIM
    whole = slice(None)
    pieces = [(nat_own, gs, whole)]
    for shard, out in ((sh_q, gq), (sh_e, ge), (sh_r, gr)):
        pieces += [(shard, out, pl.ds(0, half)), (shard, out, pl.ds(half, half))]
    n_p = len(pieces)

    def place(p, at):
        shard, out, cols = pieces[p]
        if cols is whole:
            return out.at[at]
        return out.at[at + (whole, cols)]

    def source(p):
        shard, out, cols = pieces[p]
        return shard if cols is whole else shard.at[:, cols]

    def own(p):
        return pltpu.make_async_copy(source(p), place(p, (y, c, z, x)), local_sem.at[p])

    def to_z(p, k):
        return push(source(p), place(p, (y, c, z, x)), z_send.at[p, k], z_recv.at[p, k], along_z[k])

    plan = {
        0: (0, first),
        1: (0, second),
        2: (1, second),
        3: (0, sibling),
        4: (1, sibling),
        5: (2, sibling),
        6: (3, sibling),
    }

    def move(p, slot):
        which, peer = plan[slot]
        sy, sx = sets[which]
        shard, out, cols = pieces[p]
        part = out.at[sy, c, :, sx] if cols is whole else out.at[sy, c, :, sx, :, cols]
        return push(part, part, s_send.at[p, slot], s_recv.at[p, slot], peer)

    ahead = 3

    def send_z(p):
        for k in range(n_z - 1):
            to_z(p, k).start()

    def advance(step):
        p = step
        if 0 <= p < n_p:
            own(p).wait()
            for k in range(n_z - 1):
                to_z(p, k).wait_recv()
            for slot in (0, 1, 3):
                move(p, slot).start()
            if p + ahead < n_p:
                send_z(p + ahead)
        p = step - 1
        if 0 <= p < n_p:
            move(p, 0).wait_recv()
            move(p, 2).start()
            move(p, 4).start()
        p = step - 2
        if 0 <= p < n_p:
            move(p, 1).wait_recv()
            move(p, 5).start()
            move(p, 2).wait_recv()
            move(p, 6).start()
        p = step - 3
        if 0 <= p < n_p:
            for slot in (3, 4, 5, 6):
                move(p, slot).wait_recv()

    def image(i):
        return pltpu.make_async_copy(tokens.at[t_me * n_img + i], xall.at[i], x_sem.at[i])

    def fetch_wq():
        return pltpu.make_async_copy(gq, wq, w_sem.at[0])

    @pl.when(s == 0)
    def _():
        for i in range(n_img):
            image(i).start()
        for j in range(3):
            sh_q[:, j * q_width : (j + 1) * q_width] = qkv_w[j].astype(bf16)
        sh_q[:, 3 * q_width :] = proj_w[...].T.astype(bf16)
        sh_e[...] = exp_w[...].astype(bf16)
        sh_r[...] = red_w[...].astype(bf16)
        xs[...] = jnp.zeros_like(xs)
        greet([first, second, sibling] + along_z)
        for p in range(n_p):
            own(p).start()
        for p in range(ahead):
            send_z(p)
        for step in range(6):
            advance(step)
        fetch_wq().start()
        total = jnp.zeros((NAT_ROWS, width), f32)
        for yy in range(2):
            for cc in range(2):
                for xx in range(2):
                    for zz in range(n_z):
                        total = total + gs[yy, cc, zz, xx].astype(f32)
        nat_ref[...] = total
        for i in range(n_img):
            image(i).wait()
        fetch_wq().wait()

    for grid_step, step in ((2, 6), (3, 7), (4, 8)):
        pl.when(s == grid_step)(lambda step=step: advance(step))

    @pl.when((s >= 1) & (s <= n_img))
    def _():
        xs[pl.ds(0, seq), :] = xall[s - 1]
        normed, scale = norm_stats(xs[...])
        n1_ref[...] = normed
        a1_ref[...] = (normed * nat_ref[NAT_VEC : NAT_VEC + 1, :] + nat_ref[NAT_VEC + 1 : NAT_VEC + 2, :]).astype(bf16)
        mask = key_mask(rows, seq)
        lane = lax.broadcasted_iota(jnp.int32, (rows, 128), 1)
        lse_all = jnp.where(lane == 127, scale, 0.0)
        pad = mix - q_width
        for t in range(4):
            w_t = wq[t // 2, t % 2, :, :, :, :wide].reshape(width, wide)
            qkv = (dot_nn(a1_ref[...], w_t) + nat_ref[4 + t : 5 + t, :wide]).astype(bf16)
            qkv_ref[:, t * wide : (t + 1) * wide] = qkv
            outs = [jnp.zeros((rows, pad), bf16)]
            for h in range(n_heads):
                q = qkv[:, h * HEAD_DIM : (h + 1) * HEAD_DIM]
                k = qkv[:, q_width + h * HEAD_DIM : q_width + (h + 1) * HEAD_DIM]
                v = qkv[:, 2 * q_width + h * HEAD_DIM : 2 * q_width + (h + 1) * HEAD_DIM]
                scores = jnp.where(mask, dot_nt(q, k) * (HEAD_DIM**-0.5), -1e30)
                top = jnp.max(scores, axis=-1, keepdims=True)
                e = jnp.exp(scores - top)
                total = jnp.sum(e, axis=-1, keepdims=True)
                p = (e * (1.0 / total)).astype(bf16)
                outs.append(dot_nn(p, v).astype(bf16))
                lse_all = jnp.where(lane == t * n_heads + h, top + jnp.log(total), lse_all)
            mix_ref[:, t * mix : (t + 1) * mix] = jnp.concatenate(outs, axis=1)
        lse_ref[...] = lse_all

    @pl.when(s == n_img + 1)
    def _():
        advance(9)
        for p in range(n_p):
            for k in range(n_z - 1):
                to_z(p, k).wait_send()
            for slot in plan:
                move(p, slot).wait_send()


def fore(qkv_w, proj_w, exp_w, red_w, nat_own, tokens, n_dp, n_img, rows, n_heads):
    slots, seq, width = tokens.shape
    n_z = n_dp // 2
    own_d = exp_w.shape[0]
    q3 = 3 * n_heads * HEAD_DIM
    wide, mix = -(-q3 // 128) * 128, width - (q3 // 128) * 128
    total = n_img * rows
    cfg = (n_z, n_img, seq, rows, n_heads, wide, mix)
    block = (own_d, width)
    full = (2, 2, n_z, 2)
    whole = lambda shape: pl.BlockSpec(
        shape, lambda s, nd=len(shape): (0,) * nd, pipeline_mode=pl.Buffered(1)
    )
    by_image = lambda n: pl.BlockSpec((rows, n), lambda s: (jnp.clip(s - 1, 0, n_img - 1), 0))
    anywhere = pl.BlockSpec(memory_space=pl.ANY)
    dma = pltpu.SemaphoreType.DMA
    n_p = 7
    return pl.pallas_call(
        functools.partial(fore_body, cfg),
        out_shape=[jax.ShapeDtypeStruct(full + block, bf16)] * 3
        + [
            jax.ShapeDtypeStruct((NAT_ROWS, width), f32),
            jax.ShapeDtypeStruct((total, width), bf16),
            jax.ShapeDtypeStruct((total, width), f32),
            jax.ShapeDtypeStruct((total, 4 * wide), bf16),
            jax.ShapeDtypeStruct((total, 4 * mix), bf16),
            jax.ShapeDtypeStruct((total, 128), f32),
        ],
        grid=(n_img + 2,),
        in_specs=[whole(a.shape) for a in (qkv_w, proj_w, exp_w, red_w, nat_own)] + [anywhere],
        out_specs=[anywhere] * 3
        + [whole((NAT_ROWS, width))]
        + [by_image(n) for n in (width, width, 4 * wide, 4 * mix, 128)],
        scratch_shapes=[
            pltpu.VMEM((rows, width), f32),
            pltpu.VMEM((n_img, seq, width), f32),
            pltpu.VMEM(block, bf16),
            pltpu.VMEM(block, bf16),
            pltpu.VMEM(block, bf16),
            pltpu.VMEM(full + (NAT_ROWS, width), bf16),
            pltpu.VMEM(full + block, bf16),
            dma((n_img,)),
            dma((1,)),
            dma((n_p,)),
            dma((n_p, n_z - 1)),
            dma((n_p, n_z - 1)),
            dma((n_p, 7)),
            dma((n_p, 7)),
        ],
        compiler_params=pltpu.CompilerParams(
            collective_id=0, has_side_effects=True, vmem_limit_bytes=VMEM_MAX
        ),
        name="fore",
    )(qkv_w, proj_w, exp_w, red_w, nat_own, tokens)


def middle_body(
    seq,
    where,
    x_ref,
    cot_ref,
    mix_ref,
    nat_ref,
    wq_ref,
    we_ref,
    wr_ref,
    a2_ref,
    hd_ref,
    gh_ref,
    dres_ref,
    drh_ref,
    dmix_ref,
    out_ref,
    dvec_ref,
    dbexp_ref,
    xs,
    gs,
):
    i = pl.program_id(0)

    @pl.when(i == 0)
    def _():
        xs[...] = jnp.zeros_like(xs)
        gs[...] = jnp.zeros_like(gs)
        dvec_ref[...] = jnp.zeros_like(dvec_ref)
        dbexp_ref[...] = jnp.zeros_like(dbexp_ref)

    live = jnp.where(where[0] + i < where[1], 1.0, 0.0).astype(f32)
    load_rows(x_ref, xs, seq)
    gs[pl.ds(0, seq), :] = cot_ref[0] * live
    rows, width = xs.shape
    mix = mix_ref.shape[1] // 4
    ff = we_ref.shape[2]
    att = jnp.zeros((rows, width), f32)
    for t in range(4):
        att += half_round(dot_nt(mix_ref[:, t * mix : (t + 1) * mix], wq_ref[t, :, width - mix :]))
    resid = xs[...] + att + nat_ref[NAT_VEC + 2 : NAT_VEC + 3, :]
    normed2, scale2 = norm_stats(resid)
    a2_ref[...] = (normed2 * nat_ref[NAT_VEC + 3 : NAT_VEC + 4, :] + nat_ref[NAT_VEC + 4 : NAT_VEC + 5, :]).astype(bf16)
    gh_ref[...] = gs[...].astype(bf16)
    feed = jnp.zeros((rows, width), f32)
    d_a2 = jnp.zeros((rows, width), f32)
    for t in range(4):
        pre = dot_nn(a2_ref[...], we_ref[t]) + nat_ref[t : t + 1, :ff]
        cdf = 0.5 + 0.5 * lax.erf(pre * (0.5**0.5))
        hid = (pre * cdf).astype(bf16)
        slope = cdf + pre * jnp.exp(-0.5 * pre * pre) * ((2.0 * jnp.pi) ** -0.5)
        hd_ref[:, t * ff : (t + 1) * ff] = hid
        d_pre = dot_nn(gh_ref[...], wr_ref[t]) * slope
        dbexp_ref[t, 0:1, :] += jnp.sum(d_pre, axis=0, keepdims=True)
        dph = d_pre.astype(bf16)
        hd_ref[:, (4 + t) * ff : (5 + t) * ff] = dph
        feed += half_round(dot_nt(hid, wr_ref[t]))
        d_a2 += half_round(dot_nt(dph, we_ref[t]))
    out = (resid + feed + nat_ref[NAT_VEC + 5 : NAT_VEC + 6, :]) * live
    col = width // 2
    for t in range(2):
        out_ref[t, 0] = out[:seq, t * col : (t + 1) * col].astype(bf16)
    d_resid = gs[...] + norm_back(d_a2, normed2, scale2, nat_ref[NAT_VEC + 3 : NAT_VEC + 4, :])
    dres_ref[...] = d_resid
    drh = d_resid.astype(bf16)
    drh_ref[...] = drh
    for t in range(4):
        dmix_ref[:, t * mix : (t + 1) * mix] = dot_nn(drh, wq_ref[t, :, width - mix :]).astype(bf16)
    dvec_ref[2:3, :] += jnp.sum(d_resid, axis=0, keepdims=True)
    dvec_ref[3:4, :] += jnp.sum(d_a2 * normed2, axis=0, keepdims=True)
    dvec_ref[4:5, :] += jnp.sum(d_a2, axis=0, keepdims=True)
    dvec_ref[5:6, :] += jnp.sum(gs[...], axis=0, keepdims=True)


def middle(where, tokens, cotangent, mixp, nat, wq, we, wr, n_img, rows):
    slots, seq, width = tokens.shape
    ff = we.shape[2]
    mix = mixp.shape[1]
    total = n_img * rows
    col = width // 2
    row_block = lambda n: pl.BlockSpec((rows, n), lambda i, s: (i, 0))
    whole = lambda a: pl.BlockSpec(
        a.shape, lambda i, s, nd=len(a.shape): (0,) * nd, pipeline_mode=pl.Buffered(1)
    )
    image = pl.BlockSpec((1, seq, width), lambda i, s: (s[0] + i, 0, 0))
    return pl.pallas_call(
        functools.partial(middle_body, seq),
        out_shape=[
            jax.ShapeDtypeStruct((total, width), bf16),
            jax.ShapeDtypeStruct((total, 8 * ff), bf16),
            jax.ShapeDtypeStruct((total, width), bf16),
            jax.ShapeDtypeStruct((total, width), f32),
            jax.ShapeDtypeStruct((total, width), bf16),
            jax.ShapeDtypeStruct((total, mix), bf16),
            jax.ShapeDtypeStruct((2, n_img, seq, col), bf16),
            jax.ShapeDtypeStruct((8, width), f32),
            jax.ShapeDtypeStruct((4, 8, ff), f32),
        ],
        grid_spec=pltpu.PrefetchScalarGridSpec(
            num_scalar_prefetch=1,
            grid=(n_img,),
            in_specs=[image, image, row_block(mix)] + [whole(a) for a in (nat, wq, we, wr)],
            out_specs=[
                row_block(width),
                row_block(8 * ff),
                row_block(width),
                row_block(width),
                row_block(width),
                row_block(mix),
                pl.BlockSpec((2, 1, seq, col), lambda i, s: (0, i, 0, 0)),
                pl.BlockSpec((8, width), lambda i, s: (0, 0)),
                pl.BlockSpec((4, 8, ff), lambda i, s: (0, 0, 0)),
            ],
            scratch_shapes=[pltpu.VMEM((rows, width), f32), pltpu.VMEM((rows, width), f32)],
        ),
        compiler_params=pltpu.CompilerParams(vmem_limit_bytes=VMEM_MAX),
        name="middle",
    )(where, tokens, cotangent, mixp, nat, wq, we, wr)


def attention_back(seq, n_heads, qkv_ref, lse_rows, dmix_ref, t, wide, mix):
    rows = qkv_ref.shape[0]
    q_width = n_heads * HEAD_DIM
    scale_qk = HEAD_DIM**-0.5
    mask = lax.broadcasted_iota(jnp.int32, (rows, rows), 0) < seq
    dq_t, dk, dv = [], [], []
    for h in range(n_heads):
        at = t * wide + h * HEAD_DIM
        q = qkv_ref[:, at : at + HEAD_DIM]
        k = qkv_ref[:, at + q_width : at + q_width + HEAD_DIM]
        v = qkv_ref[:, at + 2 * q_width : at + 2 * q_width + HEAD_DIM]
        m_at = (t + 1) * mix - q_width + h * HEAD_DIM
        dm = dmix_ref[:, m_at : m_at + HEAD_DIM]
        lse = lse_rows[t * n_heads + h : t * n_heads + h + 1, :]
        p = jnp.where(mask, jnp.exp(dot_nt(k, q) * scale_qk - lse), 0.0)
        dv.append(dot_nn(p.astype(bf16), dm))
        d_p = dot_nt(v, dm)
        delta = jnp.sum(p * d_p, axis=0, keepdims=True)
        ds = (p * (d_p - delta) * scale_qk).astype(bf16)
        dq_t.append(dot_tn(k, ds))
        dk.append(dot_nn(ds, q))
    dq = jnp.concatenate(dq_t, axis=0).T
    return jnp.concatenate([dq] + dk + dv + [jnp.zeros((rows, wide - 3 * q_width), f32)], axis=1)


def rear_body(cfg, *refs):
    n_z, n_img, seq, rows, n_heads, shard_rows, wide, mix, ff = cfg
    (hd_ref, mix_ref, qkv_ref, lse_ref, dmix_ref, dres_ref, n1_ref, nat_ref, wq_ref, dvec_in, dbexp_in) = refs[:11]
    gh_any, a2_any, a1_any, drh_any, out2_any = refs[11:16]
    gr_out, ge_out, gq_out, gs_out, ro_out, rg_out = refs[16:22]
    (lhs_a, lhs_b, dqs, gts) = refs[22:26]
    part, got, got2, got1, gotz = (refs[26 + 4 * k : 30 + 4 * k] for k in range(5))
    sv, sgot, sz = refs[46:49]
    (
        lhs_sem,
        load_sem,
        keep_sem,
        o_send,
        o_recv,
        g_send,
        g_recv,
        f_send,
        f_recv,
        h_send,
        h_recv,
        s_send,
        s_recv,
        z_send,
        z_recv,
        v_send,
        v_recv,
        vz_send,
        vz_recv,
    ) = refs[49:]
    half_q = gq_out.shape[1] // 2
    outs = (gr_out, ge_out, gq_out.at[:, :half_q], gq_out.at[:, half_q:])
    s = pl.program_id(0)
    n_t = 4
    base_e, base_b = n_t, 2 * n_t
    base_q = base_b + n_img
    base_t = base_q + n_t
    width = n1_ref.shape[1]
    n_dp = 2 * n_z

    dp = lax.axis_index("dp")
    t_me = lax.axis_index("tensor")
    z, x = dp // 2, dp % 2
    y, c = t_me // 2, t_me % 2
    fy, fx = 1 - 2 * y, 1 - 2 * x
    sibling = (dp, t_me + 1 - 2 * c)
    over_y = (dp, t_me + 2 * fy)
    over_x = (dp + fx, t_me)
    along_z = [(lax.rem(z + k, n_z) * 2 + x, t_me) for k in range(1, n_z)]

    def route(w):
        m = c
        first = (dp + m * fx, t_me + (1 - m) * 2 * fy)
        second = (dp + (1 - m) * fx, t_me + m * 2 * fy)
        sets = (
            (y, x),
            (y + (1 - m) * fy, x + m * fx),
            (y + m * fy, x + (1 - m) * fx),
            (1 - y, 1 - x),
        )
        return first, second, sets

    def half(w, yy):
        return push(part[w].at[1 - c, yy], got[w].at[yy], h_send.at[w, yy], h_recv.at[w, yy], sibling)

    def to_second(w, k):
        first, second, sets = route(w)
        sy, sx = sets[k]
        return push(
            part[w].at[c, sy, sx], got2[w].at[k - 2], s_send.at[w, k - 2], s_recv.at[w, k - 2], second
        )

    def to_first(w):
        first, second, sets = route(w)
        sy, sx = sets[1]
        return push(part[w].at[c, sy, sx], got1[w], s_send.at[w, 2], s_recv.at[w, 2], first)

    def to_z(w, k):
        return push(
            part[w].at[c, y, x, along_z[k][0] // 2],
            gotz[w].at[k],
            z_send.at[w, k],
            z_recv.at[w, k],
            along_z[k],
        )

    def add(w, k, other):
        sy, sx = route(w)[2][k]

        def one(i, carry):
            mine = part[w][c, sy, sx, i].astype(f32)
            part[w][c, sy, sx, i] = (mine + other(sy, sx, i).astype(f32)).astype(bf16)
            return carry

        lax.fori_loop(0, n_z, one, 0)

    def stage_b(w):
        half(w, 0).wait_recv()
        half(w, 1).wait_recv()
        for k in (3, 2, 1, 0):
            add(w, k, lambda sy, sx, i: got[w][sy, sx, i])
            if k >= 2:
                to_second(w, k).start()

    def stage_c(w):
        to_second(w, 3).wait_recv()
        add(w, 1, lambda sy, sx, i: got2[w][1, i])
        to_first(w).start()
        to_second(w, 2).wait_recv()
        add(w, 0, lambda sy, sx, i: got2[w][0, i])

    def stage_d(w):
        to_first(w).wait_recv()
        add(w, 0, lambda sy, sx, i: got1[w][i])
        for k in range(n_z - 1):
            to_z(w, k).start()

    def stage_f(w):
        total = part[w][c, y, x, z].astype(f32)
        for k in range(n_z - 1):
            to_z(w, k).wait_recv()
            total = total + gotz[w][k].astype(f32)
        outs[w][...] = total

    def small(k):
        peer = (sibling, over_x, over_y)[k]
        return push(sv.at[k], sgot.at[k], v_send.at[k], v_recv.at[k], peer)

    def small_step(k):
        small(k).wait_recv()
        sv[k + 1] = sv[k] + sgot[k]
        if k < 2:
            small(k + 1).start()
        else:
            sz[z] = sv[3]
            for j in range(n_z - 1):
                small_z(j).start()

    def small_z(j):
        return push(sv.at[3], sz.at[z], vz_send.at[j], vz_recv.at[j], along_z[j])

    def small_end():
        for j in range(n_z - 1):
            small_z(j).wait_recv()
        total = sz[0]
        for j in range(1, n_z):
            total = total + sz[j]
        gs_out[...] = total

    def load(k, src):
        return pltpu.make_async_copy(src, (lhs_a, lhs_b)[k], lhs_sem.at[k])

    def out_load():
        return pltpu.make_async_copy(out2_any, gts, load_sem.at[0])

    def out_keep():
        return pltpu.make_async_copy(gts.at[y], ro_out.at[t_me], keep_sem.at[0])

    def out_sibling():
        return push(out2_any.at[y], ro_out.at[t_me], o_send.at[0], o_recv.at[0], sibling)

    def out_y():
        return push(out2_any.at[1 - y], ro_out.at[t_me], o_send.at[1], o_recv.at[1], over_y)

    def forward(ref, slot):
        row = ref.at[t_me + 2 * fy]
        return push(row, row, f_send.at[slot], f_recv.at[slot], sibling)

    def gt_keep(i):
        return pltpu.make_async_copy(gts.at[y, i], rg_out.at[t_me, i], keep_sem.at[1 + i])

    def gt_sibling(i):
        return push(gts.at[y, i], rg_out.at[t_me, i], g_send.at[i, 0], g_recv.at[i, 0], sibling)

    def gt_y(i):
        return push(gts.at[1 - y, i], rg_out.at[t_me, i], g_send.at[i, 1], g_recv.at[i, 1], over_y)

    def at(step):
        return pl.when(s == step)

    @at(0)
    def _():
        load(0, gh_any).start()
        load(1, a2_any).start()
        out_load().start()
        greet([sibling, over_x, over_y] + along_z)
        out_y().start()
        out_sibling().start()
        sv[...] = jnp.zeros_like(sv)
        load(0, gh_any).wait()
        load(1, a2_any).wait()
        out_load().wait()
        out_keep().start()

    @at(base_e + 1)
    def _():
        stage_b(0)

    @at(base_b)
    def _():
        load(0, a1_any).start()
        load(1, drh_any).start()
        stage_b(1)
        out_keep().wait()
        out_y().wait_recv()
        forward(ro_out, 0).start()

    early = [
        (base_b + 1, lambda: stage_c(0)),
        (base_b + 3, lambda: stage_d(0)),
        (base_b + 4, lambda: stage_c(1)),
    ]
    for step, event in early:
        at(min(step, base_q))(event)

    @at(base_q)
    def _():
        stage_d(1)
        load(0, a1_any).wait()
        load(1, drh_any).wait()
        small(0).start()

    at(base_q + 1)(lambda: small_step(0))
    at(base_q + 2)(lambda: small_step(1))

    @at(base_q + 3)
    def _():
        small_step(2)

    @at(base_t)
    def _():
        stage_b(2)
        stage_b(3)
        small_end()
        stage_f(0)
        stage_f(1)
        for i in range(n_img):
            gt_y(i).wait_recv()
        forward(rg_out, 1).start()

    for step, stage in ((base_t + 1, stage_c), (base_t + 2, stage_d)):

        @at(step)
        def _(stage=stage):
            stage(2)
            stage(3)


    def put(w, t, g):
        g = g.astype(bf16)
        for d in range(n_dp):
            part[w][t % 2, t // 2, d % 2, d // 2] = g[d * shard_rows : (d + 1) * shard_rows]

    def put_q(t, g):
        put(2, t, g[:, :half_q])
        put(3, t, g[:, half_q:])

    @pl.when(s < base_e)
    def _():
        put(0, s, dot_tn(lhs_a[...], hd_ref[...]))

    @pl.when((s >= base_e) & (s < base_b))
    def _():
        put(1, s - base_e, dot_tn(lhs_b[...], hd_ref[...]))

    @pl.when((s >= base_b) & (s < base_q))
    def _():
        i = s - base_b
        d_a1 = jnp.zeros((rows, width), f32)
        lse_rows = lse_ref[...].T
        for t in range(4):
            d_all = attention_back(seq, n_heads, qkv_ref, lse_rows, dmix_ref, t, wide, mix)
            sv[0, 4 + t : 5 + t, :wide] += jnp.sum(d_all, axis=0, keepdims=True)
            d_half = d_all.astype(bf16)
            dqs[t, pl.ds(i * rows, rows), :] = d_half
            d_a1 += half_round(dot_nt(d_half, wq_ref[t, :, :wide]))
        normed, scale = n1_ref[...], lse_ref[:, 127:128]
        grad = dres_ref[...] + norm_back(d_a1, normed, scale, nat_ref[NAT_VEC : NAT_VEC + 1, :])
        col = width // 2
        for h in range(2):
            gts[h, i] = grad[:seq, h * col : (h + 1) * col].astype(bf16)
        sv[0, 8:9, :] += jnp.sum(d_a1 * normed, axis=0, keepdims=True)
        sv[0, 9:10, :] += jnp.sum(d_a1, axis=0, keepdims=True)

    @pl.when((s >= base_q) & (s < base_t))
    def _():
        t = s - base_q
        dq = dot_tn(lhs_a[...], dqs[t])
        dp_ = dot_tn(lhs_b[...], mix_ref[...])
        cut = width - mix
        put_q(
            t,
            jnp.concatenate(
                [dq[:, :cut], dq[:, cut:] + dp_[:, : wide - cut], dp_[:, wide - cut :]], axis=1
            ),
        )

    at(1)(lambda: half(0, 0).start())
    at(3)(lambda: half(0, 1).start())
    at(base_e + 1)(lambda: half(1, 0).start())
    at(base_e + 3)(lambda: half(1, 1).start())
    for i in range(n_img):

        @at(base_b + i)
        def _(i=i):
            gt_keep(i).start()
            gt_y(i).start()
            gt_sibling(i).start()

    @at(base_q - 1)
    def _():
        sv[0, 10:14, :] = dvec_in[2:6, :]
        for t in range(4):
            sv[0, t : t + 1, :] = dbexp_in[t, 0:1, :]

    for step, yy in ((base_q + 1, 0), (base_q + 3, 1)):

        @at(step)
        def _(yy=yy):
            half(2, yy).start()
            half(3, yy).start()


    @at(base_t + 3)
    def _():
        stage_f(2)
        stage_f(3)
        out_sibling().wait_recv()
        forward(ro_out, 0).wait_recv()
        for i in range(n_img):
            gt_keep(i).wait()
            gt_sibling(i).wait_recv()
        forward(rg_out, 1).wait_recv()
        out_sibling().wait_send()
        out_y().wait_send()
        for i in range(n_img):
            gt_sibling(i).wait_send()
            gt_y(i).wait_send()
        forward(ro_out, 0).wait_send()
        forward(rg_out, 1).wait_send()
        for w in range(4):
            half(w, 0).wait_send()
            half(w, 1).wait_send()
            to_second(w, 2).wait_send()
            to_second(w, 3).wait_send()
            to_first(w).wait_send()
            for k in range(n_z - 1):
                to_z(w, k).wait_send()
        for k in range(3):
            small(k).wait_send()
        for j in range(n_z - 1):
            small_z(j).wait_send()


def rear(hd, mixp, qkv, lse, dmix, dres, n1, vec, wq, dvec, dbexp, gh, a2, a1, drh, out2, n_dp, n_img, n_heads):
    total, width = n1.shape
    rows = total // n_img
    ff = hd.shape[1] // 8
    wide, mix = qkv.shape[1] // 4, mixp.shape[1] // 4
    seq, col = out2.shape[2], out2.shape[3]
    n_z = n_dp // 2
    shard_rows = width // n_dp
    n_t = 4
    base_b = 2 * n_t
    base_q = base_b + n_img
    n_steps = base_q + n_t + 4
    cfg = (n_z, n_img, seq, rows, n_heads, shard_rows, wide, mix, ff)
    image = lambda s: (jnp.clip(s - base_b, 0, n_img - 1), 0)
    by_image = lambda n: pl.BlockSpec((rows, n), image)
    whole = lambda a: pl.BlockSpec(
        a.shape, lambda s, nd=len(a.shape): (0,) * nd, pipeline_mode=pl.Buffered(1)
    )
    anywhere = pl.BlockSpec(memory_space=pl.ANY)
    resident = lambda shape: pl.BlockSpec(
        shape, lambda s, nd=len(shape): (0,) * nd, pipeline_mode=pl.Buffered(1)
    )
    block = (shard_rows, width)
    dma = pltpu.SemaphoreType.DMA
    scratch = [
        pltpu.VMEM((total, width), bf16),
        pltpu.VMEM((total, width), bf16),
        pltpu.VMEM((4, total, wide), bf16),
        pltpu.VMEM((2, n_img, seq, col), bf16),
    ]
    pieces = [block, block, (shard_rows, width // 2), (shard_rows, width // 2)]
    for lead in ((2, 2, 2, n_z), (2, 2, n_z), (2, n_z), (n_z,), (n_z - 1,)):
        scratch += [pltpu.VMEM(lead + piece, bf16) for piece in pieces]
    scratch += [
        pltpu.VMEM((4, S_ROWS, width), f32),
        pltpu.VMEM((3, S_ROWS, width), f32),
        pltpu.VMEM((n_z, S_ROWS, width), f32),
    ]
    scratch += [dma((2,)), dma((1,)), dma((1 + n_img,))]
    scratch += [dma((2,))] * 2 + [dma((n_img, 2))] * 2 + [dma((2,))] * 2
    scratch += [dma((4, 2))] * 2 + [dma((4, 3))] * 2 + [dma((4, n_z - 1))] * 2
    scratch += [dma((3,))] * 2 + [dma((n_z - 1,))] * 2
    return pl.pallas_call(
        functools.partial(rear_body, cfg),
        out_shape=[jax.ShapeDtypeStruct(block, f32)] * 3
        + [jax.ShapeDtypeStruct((S_ROWS, width), f32)]
        + [jax.ShapeDtypeStruct((n_t, n_img, seq, col), bf16)] * 2,
        grid=(n_steps,),
        in_specs=[
            pl.BlockSpec((total, ff), lambda s: (0, jnp.clip(s, 0, 2 * n_t - 1))),
            pl.BlockSpec((total, mix), lambda s: (0, jnp.clip(s - base_q, 0, n_t - 1))),
            by_image(4 * wide),
            by_image(128),
            by_image(4 * mix),
            by_image(width),
            by_image(width),
            whole(vec),
            whole(wq),
            whole(dvec),
            whole(dbexp),
        ]
        + [anywhere] * 5,
        out_specs=[resident(block)] * 3 + [resident((S_ROWS, width))] + [anywhere] * 2,
        scratch_shapes=scratch,
        compiler_params=pltpu.CompilerParams(
            collective_id=1, has_side_effects=True, vmem_limit_bytes=VMEM_MAX
        ),
        name="rear",
    )(hd, mixp, qkv, lse, dmix, dres, n1, vec, wq, dvec, dbexp, gh, a2, a1, drh, out2)


def finish_body(n_heads, where, out_ref, gt_ref, o_ref, g_ref):
    q_width = n_heads * HEAD_DIM
    for src, dst in ((out_ref, o_ref), (gt_ref, g_ref)):
        for i in range(src.shape[0]):
            both = src[i]
            picked = jnp.where(where[2] == 0, both[:, :q_width], both[:, q_width:])
            dst[i] = picked.astype(f32).T


def finish(where, got_out, got_gt, n_heads):
    n_t, n_img, seq, col = got_out.shape
    q_width = n_heads * HEAD_DIM
    slots = n_t * n_img
    src = pl.BlockSpec((n_img, seq, col), lambda i, s: (i, 0, 0))
    dst = pl.BlockSpec((n_img, q_width, seq), lambda i, s: (i, 0, 0))
    outs = pl.pallas_call(
        functools.partial(finish_body, n_heads),
        out_shape=[jax.ShapeDtypeStruct((slots, q_width, seq), f32)] * 2,
        grid_spec=pltpu.PrefetchScalarGridSpec(
            num_scalar_prefetch=1, grid=(n_t,), in_specs=[src, src], out_specs=[dst, dst]
        ),
        name="finish",
    )(where, got_out.reshape(slots, seq, col), got_gt.reshape(slots, seq, col))
    return [o.transpose(0, 2, 1) for o in outs]


def update_body(sizes, where, *refs):
    q_width, qb, eb, vb = sizes
    g_q, g_e, g_r, g_s = refs[:4]
    state, outs = refs[4:25], refs[25:]
    dp, t = where[3], where[4]
    width = g_s.shape[1]

    def columns(rows, at, n):
        return pltpu.roll(rows, lax.rem(width - at, width), 1)[:, :n]

    exp_row = g_s[pl.ds(t, 1), :]
    qv_row = g_s[pl.ds(4 + t, 1), :]
    grads = [
        None,
        g_q[:, 3 * q_width :].T,
        g_e[...],
        g_r[...],
        jnp.concatenate(
            [columns(qv_row, dp * qb, qb), columns(qv_row, 2 * q_width + dp * qb, qb)], axis=0
        ),
        columns(exp_row, dp * eb, eb),
        columns(g_s[8:24, :], dp * vb, vb)[:6],
    ]
    for k in range(7):
        master, first, second = state[3 * k : 3 * k + 3]
        dst = outs[4 * k : 4 * k + 4]
        rate, wd = (lr_matrix, decay) if k < 4 else (lr_vector, 0.0)
        if k == 0:
            for j in range(3):
                g = g_q[:, j * q_width : (j + 1) * q_width]
                dst[0][j] = g
                dst[1][j], dst[2][j], dst[3][j] = adamw(master[j], g, first[j], second[j], rate, wd)
        else:
            g = grads[k]
            dst[0][...] = g
            dst[1][...], dst[2][...], dst[3][...] = adamw(master[...], g, first[...], second[...], rate, wd)


def update(where, grads, state, q_width, qb, eb, vb):
    spec = pl.BlockSpec(memory_space=pltpu.VMEM)
    shapes = [jax.ShapeDtypeStruct(state[3 * k].shape, f32) for k in range(7) for j in range(4)]
    return pl.pallas_call(
        functools.partial(update_body, (q_width, qb, eb, vb)),
        out_shape=shapes,
        in_specs=[pl.BlockSpec(memory_space=pltpu.SMEM)] + [spec] * (len(grads) + len(state)),
        out_specs=[spec] * len(shapes),
        name="update",
    )(where, *grads, *state)


def adamw(master, grad, first, second, rate, decay_rate):
    first_new = beta_one * first + (1.0 - beta_one) * grad
    second_new = beta_two * second + (1.0 - beta_two) * grad * grad
    first_hat = first_new / (1.0 - beta_one**adam_step)
    second_hat = second_new / (1.0 - beta_two**adam_step)
    new = master - rate * (first_hat / (jnp.sqrt(second_hat) + adam_eps) + decay_rate * master)
    return (new, first_new, second_new)


def on_device(
    tokens,
    cotangent,
    counts,
    qkv_weight,
    proj_weight,
    expand_weight,
    reduce_weight,
    qv_bias,
    expand_bias,
    vectors,
    first_qkv_weight,
    second_qkv_weight,
    first_proj_weight,
    second_proj_weight,
    first_expand_weight,
    second_expand_weight,
    first_reduce_weight,
    second_reduce_weight,
    first_qv_bias,
    second_qv_bias,
    first_expand_bias,
    second_expand_bias,
    first_vectors,
    second_vectors,
):
    n_dp = lax.axis_size("dp")
    n_t = lax.axis_size("tensor")
    slots, seq, width = tokens.shape
    n_img = slots // n_t
    rows = -(-seq // 16) * 16
    q_width = qkv_weight.shape[2]
    n_heads = q_width // HEAD_DIM
    qb, eb, vb = qv_bias.shape[1], expand_bias.shape[0], vectors.shape[1]
    dp_me, t_me = lax.axis_index("dp"), lax.axis_index("tensor")

    nat = jnp.zeros((NAT_ROWS, width), f32)
    nat = lax.dynamic_update_slice(nat, expand_bias[None], (t_me, dp_me * eb))
    nat = lax.dynamic_update_slice(nat, qv_bias[:1], (4 + t_me, dp_me * qb))
    nat = lax.dynamic_update_slice(nat, qv_bias[1:], (4 + t_me, 2 * q_width + dp_me * qb))
    nat = lax.dynamic_update_slice(nat, jnp.where(t_me == 0, vectors, 0.0), (NAT_VEC, dp_me * vb))
    flip = lambda a: a.transpose(1, 0, 2)
    g_q, g_e, g_r, nat, a1, n1, qkv, mixp, lse = fore(
        flip(qkv_weight),
        proj_weight,
        expand_weight,
        reduce_weight.T,
        nat.astype(bf16),
        tokens,
        n_dp,
        n_img,
        rows,
        n_heads,
    )
    w_q, w_e, w_r = (g.reshape(n_t, width, width) for g in (g_q, g_e, g_r))
    start = t_me * n_img
    where = jnp.stack([start, counts[0], t_me % 2, dp_me, t_me]).astype(jnp.int32)
    a2, hd, gh, dres, drh, dmix, out2, dvec, dbexp = middle(
        where, tokens, cotangent, mixp, nat, w_q, w_e, w_r, n_img, rows
    )
    g_r, g_e, g_q, g_s, got_out, got_gt = rear(
        hd, mixp, qkv, lse, dmix, dres, n1, nat, w_q, dvec, dbexp, gh, a2, a1, drh, out2, n_dp, n_img, n_heads
    )
    output, grad_tokens = finish(where, got_out, got_gt, n_heads)
    row = lambda a: a[None]
    state = [flip(a) for a in (qkv_weight, first_qkv_weight, second_qkv_weight)]
    state += [proj_weight, first_proj_weight, second_proj_weight]
    state += [expand_weight, first_expand_weight, second_expand_weight]
    state += [a.T for a in (reduce_weight, first_reduce_weight, second_reduce_weight)]
    state += [qv_bias, first_qv_bias, second_qv_bias]
    state += [row(a) for a in (expand_bias, first_expand_bias, second_expand_bias)]
    state += [vectors, first_vectors, second_vectors]
    new = update(where, [g_q, g_e, g_r, g_s], state, q_width, qb, eb, vb)
    restore = [flip, None, None, lambda a: a.T, None, lambda a: a[0], None]
    results = [output, grad_tokens]
    for k in range(28):
        back_to = restore[k // 4]
        results.append(new[k] if back_to is None else back_to(new[k]))
    return tuple(results)


def solution(mesh):
    matrix = {
        "qkv": P("dp", None, "tensor"),
        "proj": P("tensor", "dp"),
        "expand": P("dp", "tensor"),
        "reduce": P("tensor", "dp"),
        "qvb": P(None, ("tensor", "dp")),
        "expb": P(("tensor", "dp")),
        "vec": P(None, "dp"),
    }
    specs = list(matrix.values())
    in_specs = [P("dp", None, None), P("dp", None, None), P("dp")] + specs
    out_specs = [P("dp", None, "tensor"), P("dp", None, "tensor")]
    for s in specs:
        in_specs += [s, s]
        out_specs += [s, s, s, s]
    return jax.shard_map(
        on_device,
        mesh=mesh,
        in_specs=tuple(in_specs),
        out_specs=tuple(out_specs),
        check_vma=False,
    )
```

```python
import functools

import jax
import jax.numpy as jnp
from jax import lax
from jax.experimental import pallas as pl
from jax.experimental.pallas import tpu as pltpu
from jax.sharding import PartitionSpec as P

HEAD_DIM = 64
f32 = jnp.float32
bf16 = jnp.bfloat16

lr_matrix = 0.006
lr_vector = 0.1
decay = 0.05
beta_one = 0.9
beta_two = 0.999
adam_eps = 1e-08
adam_step = 2.0
norm_eps = 1e-06
VMEM_MAX = 63 * 1024 * 1024


def dot_nn(a, b):
    return lax.dot_general(a, b, (((1,), (0,)), ((), ())), preferred_element_type=f32)


def dot_nt(a, b):
    return lax.dot_general(a, b, (((1,), (1,)), ((), ())), preferred_element_type=f32)


def dot_tn(a, b):
    return lax.dot_general(a, b, (((0,), (0,)), ((), ())), preferred_element_type=f32)


def half_round(v):
    return v.astype(bf16).astype(f32)


def norm_stats(rows):
    mean = jnp.mean(rows, axis=-1, keepdims=True)
    centred = rows - mean
    variance = jnp.mean(centred * centred, axis=-1, keepdims=True)
    scale = lax.rsqrt(variance + norm_eps)
    return centred * scale, scale


def norm_back(grad_in, normed, scale, gain):
    scaled = grad_in * gain
    return scale * (
        scaled
        - jnp.mean(scaled, axis=-1, keepdims=True)
        - normed * jnp.mean(scaled * normed, axis=-1, keepdims=True)
    )


def places(n_z):
    dp = lax.axis_index("dp")
    t = lax.axis_index("tensor")
    z, x = dp // 2, dp % 2
    y, c = t // 2, t % 2
    fy, fx = 1 - 2 * y, 1 - 2 * x
    first = (dp + c * fx, t + (1 - c) * 2 * fy)
    second = (dp + (1 - c) * fx, t + c * 2 * fy)
    sibling = (dp, t + 1 - 2 * c)
    sets = (
        (y, x),
        (y + (1 - c) * fy, x + c * fx),
        (y + c * fy, x + (1 - c) * fx),
        (1 - y, 1 - x),
    )
    along_z = [(lax.rem(z + k, n_z) * 2 + x, t) for k in range(1, n_z)]
    return z, x, y, c, first, second, sibling, sets, along_z


def greet(peers):
    barrier = pltpu.get_barrier_semaphore()
    for peer in peers:
        pl.semaphore_signal(barrier, inc=1, device_id=peer, device_id_type=pl.DeviceIdType.MESH)
    pl.semaphore_wait(barrier, len(peers))


def push(src, dst, send, recv, peer):
    return pltpu.make_async_remote_copy(
        src_ref=src,
        dst_ref=dst,
        send_sem=send,
        recv_sem=recv,
        device_id=peer,
        device_id_type=pl.DeviceIdType.MESH,
    )


def key_mask(rows, seq):
    return lax.broadcasted_iota(jnp.int32, (rows, rows), 1) < seq


def load_rows(src, dst, seq):
    dst[pl.ds(0, seq), :] = src[0]


S_ROWS = 24
NAT_ROWS = 16
NAT_VEC = 8


def fore_body(cfg, *refs):
    n_z, n_img, seq, rows, n_heads, wide, mix = cfg
    (qkv_w, proj_w, exp_w, red_w, nat_own, tokens) = refs[:6]
    (gq, ge, gr, nat_ref, a1_ref, n1_ref, qkv_ref, mix_ref, lse_ref) = refs[6:15]
    (xs, xall, sh_q, sh_e, sh_r, gs, wq) = refs[15:22]
    x_sem, w_sem, local_sem, z_send, z_recv, s_send, s_recv = refs[22:]
    s = pl.program_id(0)
    z, x, y, c, first, second, sibling, sets, along_z = places(n_z)
    t_me = lax.axis_index("tensor")
    width = xs.shape[1]
    half = width // 2
    q_width = n_heads * HEAD_DIM
    whole = slice(None)
    pieces = [(nat_own, gs, whole)]
    for shard, out in ((sh_q, gq), (sh_e, ge), (sh_r, gr)):
        pieces += [(shard, out, pl.ds(0, half)), (shard, out, pl.ds(half, half))]
    n_p = len(pieces)

    def place(p, at):
        shard, out, cols = pieces[p]
        if cols is whole:
            return out.at[at]
        return out.at[at + (whole, cols)]

    def source(p):
        shard, out, cols = pieces[p]
        return shard if cols is whole else shard.at[:, cols]

    def own(p):
        return pltpu.make_async_copy(source(p), place(p, (y, c, z, x)), local_sem.at[p])

    def to_z(p, k):
        return push(source(p), place(p, (y, c, z, x)), z_send.at[p, k], z_recv.at[p, k], along_z[k])

    plan = {
        0: (0, first),
        1: (0, second),
        2: (1, second),
        3: (0, sibling),
        4: (1, sibling),
        5: (2, sibling),
        6: (3, sibling),
    }

    def move(p, slot):
        which, peer = plan[slot]
        sy, sx = sets[which]
        shard, out, cols = pieces[p]
        part = out.at[sy, c, :, sx] if cols is whole else out.at[sy, c, :, sx, :, cols]
        return push(part, part, s_send.at[p, slot], s_recv.at[p, slot], peer)

    ahead = 3

    def send_z(p):
        for k in range(n_z - 1):
            to_z(p, k).start()

    def stage_a(p):
        own(p).wait()
        for k in range(n_z - 1):
            to_z(p, k).wait_recv()
        for slot in (0, 1, 3):
            move(p, slot).start()
        if p + ahead < n_p:
            send_z(p + ahead)

    def stage_b(p):
        move(p, 0).wait_recv()
        move(p, 2).start()
        move(p, 4).start()

    def stage_c(p):
        move(p, 1).wait_recv()
        move(p, 5).start()
        move(p, 2).wait_recv()
        move(p, 6).start()

    def stage_d(p):
        for slot in (3, 4, 5, 6):
            move(p, slot).wait_recv()

    def advance(step):
        for stage, p in ((stage_c, step - 2), (stage_b, step - 1), (stage_a, step), (stage_d, step - 3)):
            if 0 <= p < n_p:
                stage(p)

    def image(i):
        return pltpu.make_async_copy(tokens.at[t_me * n_img + i], xall.at[i], x_sem.at[i])

    def fetch_wq():
        return pltpu.make_async_copy(gq, wq, w_sem.at[0])

    @pl.when(s == 0)
    def _():
        for i in range(n_img):
            image(i).start()
        for j in range(3):
            sh_q[:, j * q_width : (j + 1) * q_width] = qkv_w[j].astype(bf16)
        sh_q[:, 3 * q_width :] = proj_w[...].T.astype(bf16)
        sh_e[...] = exp_w[...].astype(bf16)
        sh_r[...] = red_w[...].astype(bf16)
        xs[...] = jnp.zeros_like(xs)
        greet([first, second, sibling] + along_z)
        for p in range(n_p):
            own(p).start()
        for p in range(ahead):
            send_z(p)
        for step in range(6):
            advance(step)
        fetch_wq().start()
        total = jnp.zeros((NAT_ROWS, width), f32)
        for yy in range(2):
            for cc in range(2):
                for xx in range(2):
                    for zz in range(n_z):
                        total = total + gs[yy, cc, zz, xx].astype(f32)
        nat_ref[...] = total
        for i in range(n_img):
            image(i).wait()
        fetch_wq().wait()

    for grid_step, step in ((2, 6), (3, 7), (4, 8)):
        pl.when(s == grid_step)(lambda step=step: advance(step))

    @pl.when((s >= 1) & (s <= n_img))
    def _():
        xs[pl.ds(0, seq), :] = xall[s - 1]
        normed, scale = norm_stats(xs[...])
        n1_ref[...] = normed
        a1_ref[...] = (normed * nat_ref[NAT_VEC : NAT_VEC + 1, :] + nat_ref[NAT_VEC + 1 : NAT_VEC + 2, :]).astype(bf16)
        mask = key_mask(rows, seq)
        lane = lax.broadcasted_iota(jnp.int32, (rows, 128), 1)
        lse_all = jnp.where(lane == 127, scale, 0.0)
        pad = mix - q_width
        for t in range(4):
            w_t = wq[t // 2, t % 2, :, :, :, :wide].reshape(width, wide)
            qkv = (dot_nn(a1_ref[...], w_t) + nat_ref[4 + t : 5 + t, :wide]).astype(bf16)
            qkv_ref[:, t * wide : (t + 1) * wide] = qkv
            outs = [jnp.zeros((rows, pad), bf16)]
            for h in range(n_heads):
                q = qkv[:, h * HEAD_DIM : (h + 1) * HEAD_DIM]
                k = qkv[:, q_width + h * HEAD_DIM : q_width + (h + 1) * HEAD_DIM]
                v = qkv[:, 2 * q_width + h * HEAD_DIM : 2 * q_width + (h + 1) * HEAD_DIM]
                scores = jnp.where(mask, dot_nt(q, k) * (HEAD_DIM**-0.5), -1e30)
                top = jnp.max(scores, axis=-1, keepdims=True)
                e = jnp.exp(scores - top)
                total = jnp.sum(e, axis=-1, keepdims=True)
                p = (e * (1.0 / total)).astype(bf16)
                outs.append(dot_nn(p, v).astype(bf16))
                lse_all = jnp.where(lane == t * n_heads + h, top + jnp.log(total), lse_all)
            mix_ref[:, t * mix : (t + 1) * mix] = jnp.concatenate(outs, axis=1)
        lse_ref[...] = lse_all

    @pl.when(s == n_img + 1)
    def _():
        advance(9)
        for p in range(n_p):
            for k in range(n_z - 1):
                to_z(p, k).wait_send()
            for slot in plan:
                move(p, slot).wait_send()


def fore(qkv_w, proj_w, exp_w, red_w, nat_own, tokens, n_dp, n_img, rows, n_heads):
    slots, seq, width = tokens.shape
    n_z = n_dp // 2
    own_d = exp_w.shape[0]
    q3 = 3 * n_heads * HEAD_DIM
    wide, mix = -(-q3 // 128) * 128, width - (q3 // 128) * 128
    total = n_img * rows
    cfg = (n_z, n_img, seq, rows, n_heads, wide, mix)
    block = (own_d, width)
    full = (2, 2, n_z, 2)
    whole = lambda shape: pl.BlockSpec(
        shape, lambda s, nd=len(shape): (0,) * nd, pipeline_mode=pl.Buffered(1)
    )
    by_image = lambda n: pl.BlockSpec((rows, n), lambda s: (jnp.clip(s - 1, 0, n_img - 1), 0))
    anywhere = pl.BlockSpec(memory_space=pl.ANY)
    dma = pltpu.SemaphoreType.DMA
    n_p = 7
    return pl.pallas_call(
        functools.partial(fore_body, cfg),
        out_shape=[jax.ShapeDtypeStruct(full + block, bf16)] * 3
        + [
            jax.ShapeDtypeStruct((NAT_ROWS, width), f32),
            jax.ShapeDtypeStruct((total, width), bf16),
            jax.ShapeDtypeStruct((total, width), f32),
            jax.ShapeDtypeStruct((total, 4 * wide), bf16),
            jax.ShapeDtypeStruct((total, 4 * mix), bf16),
            jax.ShapeDtypeStruct((total, 128), f32),
        ],
        grid=(n_img + 2,),
        in_specs=[whole(a.shape) for a in (qkv_w, proj_w, exp_w, red_w, nat_own)] + [anywhere],
        out_specs=[anywhere] * 3
        + [whole((NAT_ROWS, width))]
        + [by_image(n) for n in (width, width, 4 * wide, 4 * mix, 128)],
        scratch_shapes=[
            pltpu.VMEM((rows, width), f32),
            pltpu.VMEM((n_img, seq, width), f32),
            pltpu.VMEM(block, bf16),
            pltpu.VMEM(block, bf16),
            pltpu.VMEM(block, bf16),
            pltpu.VMEM(full + (NAT_ROWS, width), bf16),
            pltpu.VMEM(full + block, bf16),
            dma((n_img,)),
            dma((1,)),
            dma((n_p,)),
            dma((n_p, n_z - 1)),
            dma((n_p, n_z - 1)),
            dma((n_p, 7)),
            dma((n_p, 7)),
        ],
        compiler_params=pltpu.CompilerParams(
            collective_id=0, has_side_effects=True, vmem_limit_bytes=VMEM_MAX
        ),
        name="fore",
    )(qkv_w, proj_w, exp_w, red_w, nat_own, tokens)


def middle_body(
    seq,
    where,
    x_ref,
    cot_ref,
    mix_ref,
    nat_ref,
    wq_ref,
    we_ref,
    wr_ref,
    a2_ref,
    hd_ref,
    gh_ref,
    dres_ref,
    drh_ref,
    dmix_ref,
    out_ref,
    dvec_ref,
    dbexp_ref,
    xs,
    gs,
):
    i = pl.program_id(0)

    @pl.when(i == 0)
    def _():
        xs[...] = jnp.zeros_like(xs)
        gs[...] = jnp.zeros_like(gs)
        dvec_ref[...] = jnp.zeros_like(dvec_ref)
        dbexp_ref[...] = jnp.zeros_like(dbexp_ref)

    live = jnp.where(where[0] + i < where[1], 1.0, 0.0).astype(f32)
    load_rows(x_ref, xs, seq)
    gs[pl.ds(0, seq), :] = cot_ref[0] * live
    rows, width = xs.shape
    mix = mix_ref.shape[1] // 4
    ff = we_ref.shape[2]
    att = jnp.zeros((rows, width), f32)
    for t in range(4):
        att += half_round(dot_nt(mix_ref[:, t * mix : (t + 1) * mix], wq_ref[t, :, width - mix :]))
    resid = xs[...] + att + nat_ref[NAT_VEC + 2 : NAT_VEC + 3, :]
    normed2, scale2 = norm_stats(resid)
    a2_ref[...] = (normed2 * nat_ref[NAT_VEC + 3 : NAT_VEC + 4, :] + nat_ref[NAT_VEC + 4 : NAT_VEC + 5, :]).astype(bf16)
    gh_ref[...] = gs[...].astype(bf16)
    feed = jnp.zeros((rows, width), f32)
    d_a2 = jnp.zeros((rows, width), f32)
    for t in range(4):
        pre = dot_nn(a2_ref[...], we_ref[t]) + nat_ref[t : t + 1, :ff]
        cdf = 0.5 + 0.5 * lax.erf(pre * (0.5**0.5))
        hid = (pre * cdf).astype(bf16)
        slope = cdf + pre * jnp.exp(-0.5 * pre * pre) * ((2.0 * jnp.pi) ** -0.5)
        hd_ref[:, t * ff : (t + 1) * ff] = hid
        d_pre = dot_nn(gh_ref[...], wr_ref[t]) * slope
        dbexp_ref[t, 0:1, :] += jnp.sum(d_pre, axis=0, keepdims=True)
        dph = d_pre.astype(bf16)
        hd_ref[:, (4 + t) * ff : (5 + t) * ff] = dph
        feed += half_round(dot_nt(hid, wr_ref[t]))
        d_a2 += half_round(dot_nt(dph, we_ref[t]))
    out = (resid + feed + nat_ref[NAT_VEC + 5 : NAT_VEC + 6, :]) * live
    col = width // 2
    for t in range(2):
        out_ref[t, 0] = out[:seq, t * col : (t + 1) * col].astype(bf16)
    d_resid = gs[...] + norm_back(d_a2, normed2, scale2, nat_ref[NAT_VEC + 3 : NAT_VEC + 4, :])
    dres_ref[...] = d_resid
    drh = d_resid.astype(bf16)
    drh_ref[...] = drh
    for t in range(4):
        dmix_ref[:, t * mix : (t + 1) * mix] = dot_nn(drh, wq_ref[t, :, width - mix :]).astype(bf16)
    dvec_ref[2:3, :] += jnp.sum(d_resid, axis=0, keepdims=True)
    dvec_ref[3:4, :] += jnp.sum(d_a2 * normed2, axis=0, keepdims=True)
    dvec_ref[4:5, :] += jnp.sum(d_a2, axis=0, keepdims=True)
    dvec_ref[5:6, :] += jnp.sum(gs[...], axis=0, keepdims=True)


def middle(where, tokens, cotangent, mixp, nat, wq, we, wr, n_img, rows):
    slots, seq, width = tokens.shape
    ff = we.shape[2]
    mix = mixp.shape[1]
    total = n_img * rows
    col = width // 2
    row_block = lambda n: pl.BlockSpec((rows, n), lambda i, s: (i, 0))
    whole = lambda a: pl.BlockSpec(
        a.shape, lambda i, s, nd=len(a.shape): (0,) * nd, pipeline_mode=pl.Buffered(1)
    )
    image = pl.BlockSpec((1, seq, width), lambda i, s: (s[0] + i, 0, 0))
    return pl.pallas_call(
        functools.partial(middle_body, seq),
        out_shape=[
            jax.ShapeDtypeStruct((total, width), bf16),
            jax.ShapeDtypeStruct((total, 8 * ff), bf16),
            jax.ShapeDtypeStruct((total, width), bf16),
            jax.ShapeDtypeStruct((total, width), f32),
            jax.ShapeDtypeStruct((total, width), bf16),
            jax.ShapeDtypeStruct((total, mix), bf16),
            jax.ShapeDtypeStruct((2, n_img, seq, col), bf16),
            jax.ShapeDtypeStruct((8, width), f32),
            jax.ShapeDtypeStruct((4, 8, ff), f32),
        ],
        grid_spec=pltpu.PrefetchScalarGridSpec(
            num_scalar_prefetch=1,
            grid=(n_img,),
            in_specs=[image, image, row_block(mix)] + [whole(a) for a in (nat, wq, we, wr)],
            out_specs=[
                row_block(width),
                row_block(8 * ff),
                row_block(width),
                row_block(width),
                row_block(width),
                row_block(mix),
                pl.BlockSpec((2, 1, seq, col), lambda i, s: (0, i, 0, 0)),
                pl.BlockSpec((8, width), lambda i, s: (0, 0)),
                pl.BlockSpec((4, 8, ff), lambda i, s: (0, 0, 0)),
            ],
            scratch_shapes=[pltpu.VMEM((rows, width), f32), pltpu.VMEM((rows, width), f32)],
        ),
        compiler_params=pltpu.CompilerParams(vmem_limit_bytes=VMEM_MAX),
        name="middle",
    )(where, tokens, cotangent, mixp, nat, wq, we, wr)


def attention_back(seq, n_heads, qkv_ref, lse_rows, dmix_ref, t, wide, mix):
    rows = qkv_ref.shape[0]
    q_width = n_heads * HEAD_DIM
    scale_qk = HEAD_DIM**-0.5
    mask = lax.broadcasted_iota(jnp.int32, (rows, rows), 0) < seq
    dq_t, dk, dv = [], [], []
    for h in range(n_heads):
        at = t * wide + h * HEAD_DIM
        q = qkv_ref[:, at : at + HEAD_DIM]
        k = qkv_ref[:, at + q_width : at + q_width + HEAD_DIM]
        v = qkv_ref[:, at + 2 * q_width : at + 2 * q_width + HEAD_DIM]
        m_at = (t + 1) * mix - q_width + h * HEAD_DIM
        dm = dmix_ref[:, m_at : m_at + HEAD_DIM]
        lse = lse_rows[t * n_heads + h : t * n_heads + h + 1, :]
        p = jnp.where(mask, jnp.exp(dot_nt(k, q) * scale_qk - lse), 0.0)
        dv.append(dot_nn(p.astype(bf16), dm))
        d_p = dot_nt(v, dm)
        delta = jnp.sum(p * d_p, axis=0, keepdims=True)
        ds = (p * (d_p - delta) * scale_qk).astype(bf16)
        dq_t.append(dot_tn(k, ds))
        dk.append(dot_nn(ds, q))
    dq = jnp.concatenate(dq_t, axis=0).T
    return jnp.concatenate([dq] + dk + dv + [jnp.zeros((rows, wide - 3 * q_width), f32)], axis=1)


def rear_body(cfg, *refs):
    n_z, n_img, seq, rows, n_heads, shard_rows, wide, mix, ff = cfg
    (hd_ref, mix_ref, qkv_ref, lse_ref, dmix_ref, dres_ref, n1_ref, nat_ref, wq_ref, dvec_in, dbexp_in) = refs[:11]
    gh_any, a2_any, a1_any, drh_any, out2_any = refs[11:16]
    gr_out, ge_out, gq_out, gs_out, ro_out, rg_out = refs[16:22]
    (lhs_a, lhs_b, dqs, gts) = refs[22:26]
    part, got, got2, got1, gotz = (refs[26 + 4 * k : 30 + 4 * k] for k in range(5))
    sv, sgot, sz = refs[46:49]
    (
        lhs_sem,
        load_sem,
        keep_sem,
        o_send,
        o_recv,
        g_send,
        g_recv,
        f_send,
        f_recv,
        h_send,
        h_recv,
        s_send,
        s_recv,
        z_send,
        z_recv,
        v_send,
        v_recv,
        vz_send,
        vz_recv,
    ) = refs[49:]
    half_q = gq_out.shape[1] // 2
    outs = (gr_out, ge_out, gq_out.at[:, :half_q], gq_out.at[:, half_q:])
    s = pl.program_id(0)
    n_t = 4
    base_e, base_b = n_t, 2 * n_t
    base_q = base_b + n_img
    base_t = base_q + n_t
    width = n1_ref.shape[1]
    n_dp = 2 * n_z

    dp = lax.axis_index("dp")
    t_me = lax.axis_index("tensor")
    z, x = dp // 2, dp % 2
    y, c = t_me // 2, t_me % 2
    fy, fx = 1 - 2 * y, 1 - 2 * x
    sibling = (dp, t_me + 1 - 2 * c)
    over_y = (dp, t_me + 2 * fy)
    over_x = (dp + fx, t_me)
    along_z = [(lax.rem(z + k, n_z) * 2 + x, t_me) for k in range(1, n_z)]

    def route(w):
        m = c
        first = (dp + m * fx, t_me + (1 - m) * 2 * fy)
        second = (dp + (1 - m) * fx, t_me + m * 2 * fy)
        sets = (
            (y, x),
            (y + (1 - m) * fy, x + m * fx),
            (y + m * fy, x + (1 - m) * fx),
            (1 - y, 1 - x),
        )
        return first, second, sets

    def half(w, yy):
        return push(part[w].at[1 - c, yy], got[w].at[yy], h_send.at[w, yy], h_recv.at[w, yy], sibling)

    def to_second(w, k):
        first, second, sets = route(w)
        sy, sx = sets[k]
        return push(
            part[w].at[c, sy, sx], got2[w].at[k - 2], s_send.at[w, k - 2], s_recv.at[w, k - 2], second
        )

    def to_first(w):
        first, second, sets = route(w)
        sy, sx = sets[1]
        return push(part[w].at[c, sy, sx], got1[w], s_send.at[w, 2], s_recv.at[w, 2], first)

    def to_z(w, k):
        return push(
            part[w].at[c, y, x, along_z[k][0] // 2],
            gotz[w].at[k],
            z_send.at[w, k],
            z_recv.at[w, k],
            along_z[k],
        )

    def add(w, k, other):
        sy, sx = route(w)[2][k]

        def one(i, carry):
            mine = part[w][c, sy, sx, i].astype(f32)
            part[w][c, sy, sx, i] = (mine + other(sy, sx, i).astype(f32)).astype(bf16)
            return carry

        lax.fori_loop(0, n_z, one, 0)

    def stage_b(w):
        half(w, 0).wait_recv()
        half(w, 1).wait_recv()
        for k in (3, 2, 1, 0):
            add(w, k, lambda sy, sx, i: got[w][sy, sx, i])
            if k >= 2:
                to_second(w, k).start()

    def stage_c(w):
        to_second(w, 3).wait_recv()
        add(w, 1, lambda sy, sx, i: got2[w][1, i])
        to_first(w).start()
        to_second(w, 2).wait_recv()
        add(w, 0, lambda sy, sx, i: got2[w][0, i])

    def stage_d(w):
        to_first(w).wait_recv()
        add(w, 0, lambda sy, sx, i: got1[w][i])
        for k in range(n_z - 1):
            to_z(w, k).start()

    def stage_f(w):
        total = part[w][c, y, x, z].astype(f32)
        for k in range(n_z - 1):
            to_z(w, k).wait_recv()
            total = total + gotz[w][k].astype(f32)
        outs[w][...] = total

    def small(k):
        peer = (sibling, over_x, over_y)[k]
        return push(sv.at[k], sgot.at[k], v_send.at[k], v_recv.at[k], peer)

    def small_step(k):
        small(k).wait_recv()
        sv[k + 1] = sv[k] + sgot[k]
        if k < 2:
            small(k + 1).start()
        else:
            sz[z] = sv[3]
            for j in range(n_z - 1):
                small_z(j).start()

    def small_z(j):
        return push(sv.at[3], sz.at[z], vz_send.at[j], vz_recv.at[j], along_z[j])

    def small_end():
        for j in range(n_z - 1):
            small_z(j).wait_recv()
        total = sz[0]
        for j in range(1, n_z):
            total = total + sz[j]
        gs_out[...] = total

    def load(k, src):
        return pltpu.make_async_copy(src, (lhs_a, lhs_b)[k], lhs_sem.at[k])

    def out_load():
        return pltpu.make_async_copy(out2_any, gts, load_sem.at[0])

    def out_keep():
        return pltpu.make_async_copy(gts.at[y], ro_out.at[t_me], keep_sem.at[0])

    def out_sibling():
        return push(out2_any.at[y], ro_out.at[t_me], o_send.at[0], o_recv.at[0], sibling)

    def out_y():
        return push(out2_any.at[1 - y], ro_out.at[t_me], o_send.at[1], o_recv.at[1], over_y)

    def forward(ref, slot):
        row = ref.at[t_me + 2 * fy]
        return push(row, row, f_send.at[slot], f_recv.at[slot], sibling)

    def gt_keep(i):
        return pltpu.make_async_copy(gts.at[y, i], rg_out.at[t_me, i], keep_sem.at[1 + i])

    def gt_sibling(i):
        return push(gts.at[y, i], rg_out.at[t_me, i], g_send.at[i, 0], g_recv.at[i, 0], sibling)

    def gt_y(i):
        return push(gts.at[1 - y, i], rg_out.at[t_me, i], g_send.at[i, 1], g_recv.at[i, 1], over_y)

    def at(step):
        return pl.when(s == step)

    @at(0)
    def _():
        load(0, gh_any).start()
        load(1, a2_any).start()
        out_load().start()
        greet([sibling, over_x, over_y] + along_z)
        out_y().start()
        out_sibling().start()
        sv[...] = jnp.zeros_like(sv)
        load(0, gh_any).wait()
        load(1, a2_any).wait()
        out_load().wait()
        out_keep().start()

    @at(base_e + 1)
    def _():
        stage_b(0)

    @at(base_b)
    def _():
        load(0, a1_any).start()
        load(1, drh_any).start()
        stage_b(1)
        out_keep().wait()
        out_y().wait_recv()
        forward(ro_out, 0).start()

    early = [
        (base_b + 1, lambda: stage_c(0)),
        (base_b + 3, lambda: stage_d(0)),
        (base_b + 4, lambda: stage_c(1)),
    ]
    for step, event in early:
        at(min(step, base_q))(event)

    @at(base_q)
    def _():
        stage_d(1)
        load(0, a1_any).wait()
        load(1, drh_any).wait()
        small(0).start()

    at(base_q + 1)(lambda: small_step(0))
    at(base_q + 2)(lambda: small_step(1))

    @at(base_q + 3)
    def _():
        small_step(2)

    @at(base_t)
    def _():
        stage_b(2)
        stage_b(3)
        small_end()
        stage_f(0)
        stage_f(1)
        for i in range(n_img):
            gt_y(i).wait_recv()
        forward(rg_out, 1).start()

    for step, stage in ((base_t + 1, stage_c), (base_t + 2, stage_d)):

        @at(step)
        def _(stage=stage):
            stage(2)
            stage(3)


    def put(w, t, g):
        g = g.astype(bf16)
        for d in range(n_dp):
            part[w][t % 2, t // 2, d % 2, d // 2] = g[d * shard_rows : (d + 1) * shard_rows]

    def put_q(t, g):
        put(2, t, g[:, :half_q])
        put(3, t, g[:, half_q:])

    @pl.when(s < base_e)
    def _():
        put(0, s, dot_tn(lhs_a[...], hd_ref[...]))

    @pl.when((s >= base_e) & (s < base_b))
    def _():
        put(1, s - base_e, dot_tn(lhs_b[...], hd_ref[...]))

    @pl.when((s >= base_b) & (s < base_q))
    def _():
        i = s - base_b
        d_a1 = jnp.zeros((rows, width), f32)
        lse_rows = lse_ref[...].T
        for t in range(4):
            d_all = attention_back(seq, n_heads, qkv_ref, lse_rows, dmix_ref, t, wide, mix)
            sv[0, 4 + t : 5 + t, :wide] += jnp.sum(d_all, axis=0, keepdims=True)
            d_half = d_all.astype(bf16)
            dqs[t, pl.ds(i * rows, rows), :] = d_half
            d_a1 += half_round(dot_nt(d_half, wq_ref[t, :, :wide]))
        normed, scale = n1_ref[...], lse_ref[:, 127:128]
        grad = dres_ref[...] + norm_back(d_a1, normed, scale, nat_ref[NAT_VEC : NAT_VEC + 1, :])
        col = width // 2
        for h in range(2):
            gts[h, i] = grad[:seq, h * col : (h + 1) * col].astype(bf16)
        sv[0, 8:9, :] += jnp.sum(d_a1 * normed, axis=0, keepdims=True)
        sv[0, 9:10, :] += jnp.sum(d_a1, axis=0, keepdims=True)

    @pl.when((s >= base_q) & (s < base_t))
    def _():
        t = s - base_q
        dq = dot_tn(lhs_a[...], dqs[t])
        dp_ = dot_tn(lhs_b[...], mix_ref[...])
        cut = width - mix
        put_q(
            t,
            jnp.concatenate(
                [dq[:, :cut], dq[:, cut:] + dp_[:, : wide - cut], dp_[:, wide - cut :]], axis=1
            ),
        )

    at(1)(lambda: half(0, 0).start())
    at(3)(lambda: half(0, 1).start())
    at(base_e + 1)(lambda: half(1, 0).start())
    at(base_e + 3)(lambda: half(1, 1).start())
    for i in range(n_img):

        @at(base_b + i)
        def _(i=i):
            gt_keep(i).start()
            gt_y(i).start()
            gt_sibling(i).start()

    @at(base_q - 1)
    def _():
        sv[0, 10:14, :] = dvec_in[2:6, :]
        for t in range(4):
            sv[0, t : t + 1, :] = dbexp_in[t, 0:1, :]

    for step, yy in ((base_q + 1, 0), (base_q + 3, 1)):

        @at(step)
        def _(yy=yy):
            half(2, yy).start()
            half(3, yy).start()


    @at(base_t + 3)
    def _():
        stage_f(2)
        stage_f(3)
        out_sibling().wait_recv()
        forward(ro_out, 0).wait_recv()
        for i in range(n_img):
            gt_keep(i).wait()
            gt_sibling(i).wait_recv()
        forward(rg_out, 1).wait_recv()
        out_sibling().wait_send()
        out_y().wait_send()
        for i in range(n_img):
            gt_sibling(i).wait_send()
            gt_y(i).wait_send()
        forward(ro_out, 0).wait_send()
        forward(rg_out, 1).wait_send()
        for w in range(4):
            half(w, 0).wait_send()
            half(w, 1).wait_send()
            to_second(w, 2).wait_send()
            to_second(w, 3).wait_send()
            to_first(w).wait_send()
            for k in range(n_z - 1):
                to_z(w, k).wait_send()
        for k in range(3):
            small(k).wait_send()
        for j in range(n_z - 1):
            small_z(j).wait_send()


def rear(hd, mixp, qkv, lse, dmix, dres, n1, vec, wq, dvec, dbexp, gh, a2, a1, drh, out2, n_dp, n_img, n_heads):
    total, width = n1.shape
    rows = total // n_img
    ff = hd.shape[1] // 8
    wide, mix = qkv.shape[1] // 4, mixp.shape[1] // 4
    seq, col = out2.shape[2], out2.shape[3]
    n_z = n_dp // 2
    shard_rows = width // n_dp
    n_t = 4
    base_b = 2 * n_t
    base_q = base_b + n_img
    n_steps = base_q + n_t + 4
    cfg = (n_z, n_img, seq, rows, n_heads, shard_rows, wide, mix, ff)
    image = lambda s: (jnp.clip(s - base_b, 0, n_img - 1), 0)
    by_image = lambda n: pl.BlockSpec((rows, n), image)
    whole = lambda a: pl.BlockSpec(
        a.shape, lambda s, nd=len(a.shape): (0,) * nd, pipeline_mode=pl.Buffered(1)
    )
    anywhere = pl.BlockSpec(memory_space=pl.ANY)
    resident = lambda shape: pl.BlockSpec(
        shape, lambda s, nd=len(shape): (0,) * nd, pipeline_mode=pl.Buffered(1)
    )
    block = (shard_rows, width)
    dma = pltpu.SemaphoreType.DMA
    scratch = [
        pltpu.VMEM((total, width), bf16),
        pltpu.VMEM((total, width), bf16),
        pltpu.VMEM((4, total, wide), bf16),
        pltpu.VMEM((2, n_img, seq, col), bf16),
    ]
    pieces = [block, block, (shard_rows, width // 2), (shard_rows, width // 2)]
    for lead in ((2, 2, 2, n_z), (2, 2, n_z), (2, n_z), (n_z,), (n_z - 1,)):
        scratch += [pltpu.VMEM(lead + piece, bf16) for piece in pieces]
    scratch += [
        pltpu.VMEM((4, S_ROWS, width), f32),
        pltpu.VMEM((3, S_ROWS, width), f32),
        pltpu.VMEM((n_z, S_ROWS, width), f32),
    ]
    scratch += [dma((2,)), dma((1,)), dma((1 + n_img,))]
    scratch += [dma((2,))] * 2 + [dma((n_img, 2))] * 2 + [dma((2,))] * 2
    scratch += [dma((4, 2))] * 2 + [dma((4, 3))] * 2 + [dma((4, n_z - 1))] * 2
    scratch += [dma((3,))] * 2 + [dma((n_z - 1,))] * 2
    return pl.pallas_call(
        functools.partial(rear_body, cfg),
        out_shape=[jax.ShapeDtypeStruct(block, f32)] * 3
        + [jax.ShapeDtypeStruct((S_ROWS, width), f32)]
        + [jax.ShapeDtypeStruct((n_t, n_img, seq, col), bf16)] * 2,
        grid=(n_steps,),
        in_specs=[
            pl.BlockSpec((total, ff), lambda s: (0, jnp.clip(s, 0, 2 * n_t - 1))),
            pl.BlockSpec((total, mix), lambda s: (0, jnp.clip(s - base_q, 0, n_t - 1))),
            by_image(4 * wide),
            by_image(128),
            by_image(4 * mix),
            by_image(width),
            by_image(width),
            whole(vec),
            whole(wq),
            whole(dvec),
            whole(dbexp),
        ]
        + [anywhere] * 5,
        out_specs=[resident(block)] * 3 + [resident((S_ROWS, width))] + [anywhere] * 2,
        scratch_shapes=scratch,
        compiler_params=pltpu.CompilerParams(
            collective_id=1, has_side_effects=True, vmem_limit_bytes=VMEM_MAX
        ),
        name="rear",
    )(hd, mixp, qkv, lse, dmix, dres, n1, vec, wq, dvec, dbexp, gh, a2, a1, drh, out2)


def finish_body(n_heads, where, out_ref, gt_ref, o_ref, g_ref):
    q_width = n_heads * HEAD_DIM
    for src, dst in ((out_ref, o_ref), (gt_ref, g_ref)):
        for i in range(src.shape[0]):
            both = src[i]
            picked = jnp.where(where[2] == 0, both[:, :q_width], both[:, q_width:])
            dst[i] = picked.astype(f32).T


def finish(where, got_out, got_gt, n_heads):
    n_t, n_img, seq, col = got_out.shape
    q_width = n_heads * HEAD_DIM
    slots = n_t * n_img
    src = pl.BlockSpec((n_img, seq, col), lambda i, s: (i, 0, 0))
    dst = pl.BlockSpec((n_img, q_width, seq), lambda i, s: (i, 0, 0))
    outs = pl.pallas_call(
        functools.partial(finish_body, n_heads),
        out_shape=[jax.ShapeDtypeStruct((slots, q_width, seq), f32)] * 2,
        grid_spec=pltpu.PrefetchScalarGridSpec(
            num_scalar_prefetch=1, grid=(n_t,), in_specs=[src, src], out_specs=[dst, dst]
        ),
        name="finish",
    )(where, got_out.reshape(slots, seq, col), got_gt.reshape(slots, seq, col))
    return [o.transpose(0, 2, 1) for o in outs]


def update_body(sizes, where, *refs):
    q_width, qb, eb, vb = sizes
    g_q, g_e, g_r, g_s = refs[:4]
    state, outs = refs[4:25], refs[25:]
    dp, t = where[3], where[4]
    width = g_s.shape[1]

    def columns(rows, at, n):
        return pltpu.roll(rows, lax.rem(width - at, width), 1)[:, :n]

    exp_row = g_s[pl.ds(t, 1), :]
    qv_row = g_s[pl.ds(4 + t, 1), :]
    grads = [
        None,
        g_q[:, 3 * q_width :].T,
        g_e[...],
        g_r[...],
        jnp.concatenate(
            [columns(qv_row, dp * qb, qb), columns(qv_row, 2 * q_width + dp * qb, qb)], axis=0
        ),
        columns(exp_row, dp * eb, eb),
        columns(g_s[8:24, :], dp * vb, vb)[:6],
    ]
    for k in range(7):
        master, first, second = state[3 * k : 3 * k + 3]
        dst = outs[4 * k : 4 * k + 4]
        rate, wd = (lr_matrix, decay) if k < 4 else (lr_vector, 0.0)
        if k == 0:
            for j in range(3):
                g = g_q[:, j * q_width : (j + 1) * q_width]
                dst[0][j] = g
                dst[1][j], dst[2][j], dst[3][j] = adamw(master[j], g, first[j], second[j], rate, wd)
        else:
            g = grads[k]
            dst[0][...] = g
            dst[1][...], dst[2][...], dst[3][...] = adamw(master[...], g, first[...], second[...], rate, wd)


def update(where, grads, state, q_width, qb, eb, vb):
    spec = pl.BlockSpec(memory_space=pltpu.VMEM)
    shapes = [jax.ShapeDtypeStruct(state[3 * k].shape, f32) for k in range(7) for j in range(4)]
    return pl.pallas_call(
        functools.partial(update_body, (q_width, qb, eb, vb)),
        out_shape=shapes,
        in_specs=[pl.BlockSpec(memory_space=pltpu.SMEM)] + [spec] * (len(grads) + len(state)),
        out_specs=[spec] * len(shapes),
        name="update",
    )(where, *grads, *state)


def adamw(master, grad, first, second, rate, decay_rate):
    first_new = beta_one * first + (1.0 - beta_one) * grad
    second_new = beta_two * second + (1.0 - beta_two) * grad * grad
    first_hat = first_new / (1.0 - beta_one**adam_step)
    second_hat = second_new / (1.0 - beta_two**adam_step)
    new = master - rate * (first_hat / (jnp.sqrt(second_hat) + adam_eps) + decay_rate * master)
    return (new, first_new, second_new)


def on_device(
    tokens,
    cotangent,
    counts,
    qkv_weight,
    proj_weight,
    expand_weight,
    reduce_weight,
    qv_bias,
    expand_bias,
    vectors,
    first_qkv_weight,
    second_qkv_weight,
    first_proj_weight,
    second_proj_weight,
    first_expand_weight,
    second_expand_weight,
    first_reduce_weight,
    second_reduce_weight,
    first_qv_bias,
    second_qv_bias,
    first_expand_bias,
    second_expand_bias,
    first_vectors,
    second_vectors,
):
    n_dp = lax.axis_size("dp")
    n_t = lax.axis_size("tensor")
    slots, seq, width = tokens.shape
    n_img = slots // n_t
    rows = -(-seq // 16) * 16
    q_width = qkv_weight.shape[2]
    n_heads = q_width // HEAD_DIM
    qb, eb, vb = qv_bias.shape[1], expand_bias.shape[0], vectors.shape[1]
    dp_me, t_me = lax.axis_index("dp"), lax.axis_index("tensor")

    nat = jnp.zeros((NAT_ROWS, width), f32)
    nat = lax.dynamic_update_slice(nat, expand_bias[None], (t_me, dp_me * eb))
    nat = lax.dynamic_update_slice(nat, qv_bias[:1], (4 + t_me, dp_me * qb))
    nat = lax.dynamic_update_slice(nat, qv_bias[1:], (4 + t_me, 2 * q_width + dp_me * qb))
    nat = lax.dynamic_update_slice(nat, jnp.where(t_me == 0, vectors, 0.0), (NAT_VEC, dp_me * vb))
    flip = lambda a: a.transpose(1, 0, 2)
    g_q, g_e, g_r, nat, a1, n1, qkv, mixp, lse = fore(
        flip(qkv_weight),
        proj_weight,
        expand_weight,
        reduce_weight.T,
        nat.astype(bf16),
        tokens,
        n_dp,
        n_img,
        rows,
        n_heads,
    )
    w_q, w_e, w_r = (g.reshape(n_t, width, width) for g in (g_q, g_e, g_r))
    start = t_me * n_img
    where = jnp.stack([start, counts[0], t_me % 2, dp_me, t_me]).astype(jnp.int32)
    a2, hd, gh, dres, drh, dmix, out2, dvec, dbexp = middle(
        where, tokens, cotangent, mixp, nat, w_q, w_e, w_r, n_img, rows
    )
    g_r, g_e, g_q, g_s, got_out, got_gt = rear(
        hd, mixp, qkv, lse, dmix, dres, n1, nat, w_q, dvec, dbexp, gh, a2, a1, drh, out2, n_dp, n_img, n_heads
    )
    output, grad_tokens = finish(where, got_out, got_gt, n_heads)
    row = lambda a: a[None]
    state = [flip(a) for a in (qkv_weight, first_qkv_weight, second_qkv_weight)]
    state += [proj_weight, first_proj_weight, second_proj_weight]
    state += [expand_weight, first_expand_weight, second_expand_weight]
    state += [a.T for a in (reduce_weight, first_reduce_weight, second_reduce_weight)]
    state += [qv_bias, first_qv_bias, second_qv_bias]
    state += [row(a) for a in (expand_bias, first_expand_bias, second_expand_bias)]
    state += [vectors, first_vectors, second_vectors]
    new = update(where, [g_q, g_e, g_r, g_s], state, q_width, qb, eb, vb)
    restore = [flip, None, None, lambda a: a.T, None, lambda a: a[0], None]
    results = [output, grad_tokens]
    for k in range(28):
        back_to = restore[k // 4]
        results.append(new[k] if back_to is None else back_to(new[k]))
    return tuple(results)


def solution(mesh):
    matrix = {
        "qkv": P("dp", None, "tensor"),
        "proj": P("tensor", "dp"),
        "expand": P("dp", "tensor"),
        "reduce": P("tensor", "dp"),
        "qvb": P(None, ("tensor", "dp")),
        "expb": P(("tensor", "dp")),
        "vec": P(None, "dp"),
    }
    specs = list(matrix.values())
    in_specs = [P("dp", None, None), P("dp", None, None), P("dp")] + specs
    out_specs = [P("dp", None, "tensor"), P("dp", None, "tensor")]
    for s in specs:
        in_specs += [s, s]
        out_specs += [s, s, s, s]
    return jax.shard_map(
        on_device,
        mesh=mesh,
        in_specs=tuple(in_specs),
        out_specs=tuple(out_specs),
        check_vma=False,
    )
```
